8 devices in a mesh: data: 4 (over z, y, x), stage: 2 (over core).
Axes of the slice: x: 2, y: 2, z: 1, core: 2. Of those that a mesh axis runs over, the one named last changes fastest.
Arguments:
- x_in: bfloat16 [4, 64, 8, 2048], P(None, 'data')
- g_out: bfloat16 [4, 64, 8, 2048], P(None, 'data')
- w_gate: bfloat16 [2, 2, 2048, 5632], P('stage', None, 'data')
- w_in: bfloat16 [2, 2, 2048, 5632], P('stage', None, 'data')
- w_out: bfloat16 [2, 2, 5632, 2048], P('stage', None, 'data')
Outputs:
- output 1: bfloat16 [4, 64, 8, 2048], P(None, 'data')
- output 2: float32 [2, 2, 2048, 5632], P('stage', None, 'data')
- output 3: float32 [2, 2, 2048, 5632], P('stage', None, 'data')
- output 4: float32 [2, 2, 5632, 2048], P('stage', None, 'data')
All inputs are finite; a program needn't handle non-finite values.
Results may differ from the reference program's by a relative error of at most 0.0184203.
Values are sent between devices in bfloat16 or wider.
A program may use at most 1 GiB of HBM per device.

```python
import jax
import jax.numpy as jnp
from jax import lax

N_DATA = 4
N_STAGES = 2
LAYERS_STAGE = 2
D_MODEL = 2048
D_FF = 5632
MICRO_BATCHES = 4
BATCH_MICRO = 16
SEQ_LEN = 8
EPS = 1e-6


def setup_inputs(seed: int = 0) -> dict:
    key = jax.random.key(seed)
    k_x, k_g, k_gate, k_in, k_out = jax.random.split(key, 5)
    act_shape = (MICRO_BATCHES, N_DATA * BATCH_MICRO, SEQ_LEN, D_MODEL)
    up_shape = (N_STAGES, LAYERS_STAGE, D_MODEL, D_FF)
    down_shape = (N_STAGES, LAYERS_STAGE, D_FF, D_MODEL)
    x_in = jax.random.normal(k_x, act_shape, jnp.float32).astype(jnp.bfloat16)
    g_out = jax.random.normal(k_g, act_shape, jnp.float32).astype(jnp.bfloat16)
    w_gate = (jax.random.normal(k_gate, up_shape, jnp.float32) * D_MODEL ** -0.5).astype(jnp.bfloat16)
    w_in = (jax.random.normal(k_in, up_shape, jnp.float32) * D_MODEL ** -0.5).astype(jnp.bfloat16)
    w_out = (jax.random.normal(k_out, down_shape, jnp.float32) * (0.7 * D_FF ** -0.5)).astype(jnp.bfloat16)
    return {"x_in": x_in, "g_out": g_out, "w_gate": w_gate, "w_in": w_in, "w_out": w_out}


def rms_parts(h_rows):
    h_f32 = h_rows.astype(jnp.float32)
    inv_rms = lax.rsqrt(jnp.mean(h_f32 * h_f32, axis=-1, keepdims=True) + EPS)
    return h_f32 * inv_rms, inv_rms


def layer_forward(h_rows, gate_w, in_w, out_w):
    normed_f, inv_rms = rms_parts(h_rows)
    normed = normed_f.astype(jnp.bfloat16)
    gate_pre = jnp.dot(normed, gate_w, preferred_element_type=jnp.float32)
    up_pre = jnp.dot(normed, in_w, preferred_element_type=jnp.float32)
    act = (gate_pre * jax.nn.sigmoid(gate_pre) * up_pre).astype(jnp.bfloat16)
    branch = jnp.dot(act, out_w, preferred_element_type=jnp.float32)
    return h_rows + branch.astype(jnp.bfloat16)


def layer_backward(h_rows, d_out, gate_w, in_w, out_w):
    normed_f, inv_rms = rms_parts(h_rows)
    normed = normed_f.astype(jnp.bfloat16)
    gate_pre = jnp.dot(normed, gate_w, preferred_element_type=jnp.float32)
    up_pre = jnp.dot(normed, in_w, preferred_element_type=jnp.float32)
    gate_sig = jax.nn.sigmoid(gate_pre)
    silu_val = gate_pre * gate_sig
    act = (silu_val * up_pre).astype(jnp.bfloat16)
    d_act = jnp.dot(d_out, out_w.T, preferred_element_type=jnp.float32)
    d_out_w = jnp.dot(act.T, d_out, preferred_element_type=jnp.float32)
    d_gate = (d_act * up_pre * gate_sig * (1.0 + gate_pre * (1.0 - gate_sig))).astype(jnp.bfloat16)
    d_up = (d_act * silu_val).astype(jnp.bfloat16)
    d_gate_w = jnp.dot(normed.T, d_gate, preferred_element_type=jnp.float32)
    d_in_w = jnp.dot(normed.T, d_up, preferred_element_type=jnp.float32)
    d_norm = jnp.dot(d_gate, gate_w.T, preferred_element_type=jnp.float32) + jnp.dot(d_up, in_w.T, preferred_element_type=jnp.float32)
    d_res = inv_rms * (d_norm - normed_f * jnp.mean(d_norm * normed_f, axis=-1, keepdims=True))
    d_h = (d_out.astype(jnp.float32) + d_res).astype(jnp.bfloat16)
    return d_h, d_gate_w, d_in_w, d_out_w


def reference(x_in, g_out, w_gate, w_in, w_out):
    n_layers = N_STAGES * LAYERS_STAGE
    rows = N_DATA * BATCH_MICRO * SEQ_LEN
    gate_all = w_gate.reshape(n_layers, D_MODEL, D_FF)
    in_all = w_in.reshape(n_layers, D_MODEL, D_FF)
    out_all = w_out.reshape(n_layers, D_FF, D_MODEL)

    def fwd_step(h_cur, weights):
        gate_w, in_w, out_w = weights
        return layer_forward(h_cur, gate_w, in_w, out_w), h_cur

    def bwd_step(d_cur, layer_vals):
        h_saved, gate_w, in_w, out_w = layer_vals
        d_prev, d_gate_w, d_in_w, d_out_w = layer_backward(h_saved, d_cur, gate_w, in_w, out_w)
        return d_prev, (d_gate_w, d_in_w, d_out_w)

    def micro_step(grad_sums, pair):
        x_mb, g_mb = pair
        unused, saved = lax.scan(fwd_step, x_mb.reshape(rows, D_MODEL), (gate_all, in_all, out_all))
        d_first, layer_grads = lax.scan(bwd_step, g_mb.reshape(rows, D_MODEL), (saved, gate_all, in_all, out_all), reverse=True)
        new_sums = tuple(grad_sum + grad_new for grad_sum, grad_new in zip(grad_sums, layer_grads))
        return new_sums, d_first.reshape(x_mb.shape)

    zero_up = jnp.zeros((n_layers, D_MODEL, D_FF), jnp.float32)
    zero_down = jnp.zeros((n_layers, D_FF, D_MODEL), jnp.float32)
    grad_sums, dx_in = lax.scan(micro_step, (zero_up, zero_up, zero_down), (x_in, g_out))
    return (dx_in, grad_sums[0].reshape(w_gate.shape), grad_sums[1].reshape(w_in.shape), grad_sums[2].reshape(w_out.shape))
```

```python
import jax
import jax.numpy as jnp
from jax import lax
from jax.experimental import pallas as pl
from jax.experimental.pallas import tpu as pltpu
from jax.sharding import PartitionSpec as P

EPS = 1e-6
BF = jnp.bfloat16
F32 = jnp.float32
MESH = pl.DeviceIdType.MESH

NL = 4
NM = 4
OWN = 64
ROWS = 512
D = 2048
FS = 1408
F2C = 2 * FS
MS = 512


def mm(lhs, rhs, ld=1, rd=0):
    return lax.dot_general(lhs, rhs, (((ld,), (rd,)), ((), ())), preferred_element_type=F32)


def col_tiles(total, tile, body):
    full = total // tile

    def step(idx, carry):
        body(pl.multiple_of(idx * tile, tile), tile)
        return carry

    lax.fori_loop(0, full, step, 0)
    if total % tile:
        body(full * tile, total % tile)


def kernel(x_ref, g_ref, wg_ref, wu_ref, wo_ref,
           dx_ref, dwg_ref, dwu_ref, dwo_ref, WGU, WO, XALL, AB, RC, RB, WST,
           gu, wo, nb, ab, dab, sall, part, two, tc, tb, hown, eown, nown, wst,
           ls, w_t2r, w_br, w_ar, w_abr, w_or, w_s, w_os, ag_b, ag_a, ag_c0, ag_c1, ag_s,
           rc_r, rc_s, rb_r, rb_s, g_b, g_c, g_o, g_bs, g_cs, dx_r, dx_s):
    d = lax.axis_index("data")
    c = lax.axis_index("stage")
    x = d % 2
    y = d // 2

    def role(layer):
        r = layer % 2
        al = x + r * (y - x)
        be = y + r * (x - y)
        return r, al, be

    def chip(r, al, be):
        return be * (2 - r) + al * (1 + r)

    def nbr(layer):
        r, al, be = role(layer)
        return chip(r, 1 - al, be), chip(r, al, 1 - be)

    def rcopy(src, dst, ssem, rsem, dev):
        return pltpu.make_async_remote_copy(src_ref=src, dst_ref=dst, send_sem=ssem, recv_sem=rsem, device_id=dev, device_id_type=MESH)

    def wait_for(region, sem):
        pltpu.make_async_copy(region, region, sem).wait()

    bar = pltpu.get_barrier_semaphore()
    for dd in range(1, 4):
        for cc in range(2):
            pl.semaphore_signal(bar, inc=1, device_id=((d + dd) % 4, cc), device_id_type=MESH)
    pl.semaphore_signal(bar, inc=1, device_id=(d, 1 - c), device_id_type=MESH)
    pl.semaphore_wait(bar, 7)

    def blk(ref, k, fs, lo, n):
        return ref.at[k, pl.ds(lo, n), pl.ds(pl.multiple_of(fs * FS, 128), FS)]

    def w_dst(l, row, wi, n):
        return WGU.at[l, pl.ds(row, n), pl.ds(wi * FS, FS)]

    def w_core(l):
        p, k = l // 2, l % 2
        r, al, be = role(l)
        row = pl.multiple_of(d * MS, MS)

        @pl.when(c == p)
        def _():
            for wi, ref in enumerate((wg_ref, wu_ref)):
                rcopy(blk(ref, k, chip(r, 1 - p, be), 0, MS), w_dst(l, row, wi, MS), w_s.at[l, 0], w_t2r.at[l], (d, 1 - c)).start()

    def w_split(l):
        p, k = l // 2, l % 2
        r, al, be = role(l)
        row = pl.multiple_of(d * MS, MS)
        bn = chip(r, al, 1 - be)

        @pl.when(c == p)
        def _():
            for half in range(2):
                for wi, ref in enumerate((wg_ref, wu_ref)):
                    for cc in range(2):
                        rcopy(blk(ref, k, chip(r, cc, 1 - be), half * 256, 256), w_dst(l, row + half * 256, wi, 256), w_s.at[l, 1], w_br.at[l, wi, half], (bn, cc)).start()

    def w_pair(l):
        p, k = l // 2, l % 2
        r, al, be = role(l)
        row = pl.multiple_of(d * MS, MS)
        an = chip(r, 1 - al, be)

        @pl.when(c == p)
        def _():
            for wi, ref in enumerate((wg_ref, wu_ref)):
                for cc in range(2):
                    rcopy(blk(ref, k, chip(r, cc, be), 0, MS), w_dst(l, row, wi, MS), w_s.at[l, 2], w_ar.at[l], (an, cc)).start()

    def w_fwd(l):
        r, al, be = role(l)
        an, bn = nbr(l)
        row = pl.multiple_of(bn * MS, MS)
        for half in range(2):
            for wi in range(2):
                src = w_dst(l, row + half * 256, wi, 256)
                wait_for(src, w_br.at[l, wi, half])
                rcopy(src, src, w_s.at[l, 3], w_abr.at[l], (an, c)).start()

    def w_down(l):
        p, k = l // 2, l % 2
        r, al, be = role(l)
        an = chip(r, 1 - al, be)

        @pl.when(c == p)
        def _():
            @pl.when(al != p)
            def _():
                rcopy(wo_ref.at[k], WO.at[l], w_os.at[l, 0], w_or.at[l], (d, al)).start()

            for q in range(4):
                rows = pl.ds(q * 352, 352)
                rcopy(wo_ref.at[k, rows], WO.at[l, rows], w_os.at[l, 1], w_or.at[l], (an, al)).start()

    def w_wait_gu(l):
        p = l // 2
        r, al, be = role(l)
        an, bn = nbr(l)
        abn = chip(r, 1 - al, 1 - be)

        @pl.when(c != p)
        def _():
            wait_for(WGU.at[l, pl.ds(pl.multiple_of(d * MS, MS), MS)], w_t2r.at[l])

        wait_for(WGU.at[l, pl.ds(pl.multiple_of(an * MS, MS), MS)], w_ar.at[l])
        wait_for(WGU.at[l, pl.ds(pl.multiple_of(abn * MS, MS), MS)], w_abr.at[l])

    def w_wait_o(l):
        p = l // 2
        r, al, be = role(l)

        @pl.when(jnp.logical_not(jnp.logical_and(c == al, c == p)))
        def _():
            wait_for(WO.at[l], w_or.at[l])

    def load_gu(l):
        p, k = l // 2, l % 2
        r, al, be = role(l)
        for dd in range(1, 4):
            row = pl.multiple_of(((d + dd) % 4) * MS, MS)
            pltpu.make_async_copy(WGU.at[l, pl.ds(row, MS)], gu.at[pl.ds(row, MS)], ls.at[0]).start()
        row = pl.multiple_of(d * MS, MS)

        @pl.when(c == p)
        def _():
            for wi, ref in enumerate((wg_ref, wu_ref)):
                pltpu.make_async_copy(blk(ref, k, chip(r, c, be), 0, MS), gu.at[pl.ds(row, MS), pl.ds(wi * FS, FS)], ls.at[0]).start()

        @pl.when(c != p)
        def _():
            pltpu.make_async_copy(WGU.at[l, pl.ds(row, MS)], gu.at[pl.ds(row, MS)], ls.at[0]).start()

    def load_o(l):
        p, k = l // 2, l % 2
        r, al, be = role(l)
        mine = jnp.logical_and(c == al, c == p)

        @pl.when(mine)
        def _():
            pltpu.make_async_copy(wo_ref.at[k], wo, ls.at[1]).start()

        @pl.when(jnp.logical_not(mine))
        def _():
            pltpu.make_async_copy(WO.at[l], wo, ls.at[1]).start()

    def slot(ph, m, lo, n):
        return XALL.at[ph, m, pl.ds(lo * OWN, n * OWN)]

    def ag_start(ph, layer, m, src):
        an, bn = nbr(layer)
        pltpu.make_async_copy(src, slot(ph, m, 0, 1), ls.at[2]).start()
        rcopy(src, slot(ph, m, 1, 1), ag_s.at[ph, m], ag_b.at[ph, m], (bn, c)).start()
        rcopy(src, slot(ph, m, 4, 1), ag_s.at[ph, m], ag_a.at[ph, m], (an, c)).start()
        wait_for(slot(ph, m, 0, 1), ls.at[2])

    def ag_mid(ph, layer, m):
        an, bn = nbr(layer)
        wait_for(slot(ph, m, 1, 1), ag_b.at[ph, m])
        rcopy(slot(ph, m, 1, 1), slot(ph, m, 5, 1), ag_s.at[ph, m], ag_a.at[ph, m], (an, c)).start()
        rcopy(slot(ph, m, 0, 2), slot(ph, m, 2, 2), ag_s.at[ph, m], ag_c0.at[ph, m], (d, 1 - c)).start()

    def ag_end(ph, m):
        wait_for(slot(ph, m, 4, 2), ag_a.at[ph, m])
        rcopy(slot(ph, m, 4, 2), slot(ph, m, 6, 2), ag_s.at[ph, m], ag_c1.at[ph, m], (d, 1 - c)).start()

    def ag_load(ph, m, buf, sem):
        wait_for(slot(ph, m, 2, 2), ag_c0.at[ph, m])
        wait_for(slot(ph, m, 6, 2), ag_c1.at[ph, m])
        return pltpu.make_async_copy(XALL.at[ph, m], buf, sem)

    def ag_sent(ph, m):
        wait_for(slot(ph, m, 0, 7), ag_s.at[ph, m])

    def norm(h_rows):
        h_f = h_rows.astype(F32)
        inv = lax.rsqrt(jnp.mean(h_f * h_f, axis=-1, keepdims=True) + EPS)
        return h_f * inv, inv

    def rs_core(ph, m):
        rcopy(part, RC.at[ph, m], rc_s.at[ph, m], rc_r.at[ph, m], (d, 1 - c)).start()

    def rs_split(ph, layer, m):
        an, bn = nbr(layer)
        wait_for(RC.at[ph, m], rc_r.at[ph, m])
        cp = pltpu.make_async_copy(RC.at[ph, m], tc, ls.at[3])
        cp.start()
        cp.wait()
        two[m] = two[m] + tc[...]
        rcopy(two.at[m, pl.ds(OWN, OWN)], RB.at[ph, m], rb_s.at[ph, m], rb_r.at[ph, m], (bn, c)).start()

    def rs_total(ph, m):
        wait_for(RB.at[ph, m], rb_r.at[ph, m])
        cp = pltpu.make_async_copy(RB.at[ph, m], tb, ls.at[4])
        cp.start()
        cp.wait()
        return two[m, pl.ds(0, OWN)] + tb[...]

    def rs_ready(ph, m):
        first = jnp.logical_and(ph == 0, m == 0)
        pph = jnp.where(m == 0, ph - 1, ph)
        pm = jnp.where(m == 0, NM - 1, m - 1)

        @pl.when(jnp.logical_not(first))
        def _():
            wait_for(part, rc_s.at[pph, pm])

        @pl.when(ph > 0)
        def _():
            wait_for(two.at[m, pl.ds(OWN, OWN)], rb_s.at[ph - 1, m])

    def f1(layer, m):
        cp = ag_load(layer, m, nb, ls.at[5])
        cp.start()
        cp.wait()

        def tile(lo, n):
            ab[:, pl.ds(lo, n)] = mm(nb[...], gu[:, pl.ds(lo, n)])

        col_tiles(F2C, 256, tile)
        pltpu.make_async_copy(ab, AB.at[layer, m], ls.at[6]).start()

    def f1_out(layer, m):
        def act(lo, n):
            a_pre = ab[pl.ds(0, 256), pl.ds(lo, n)]
            b_pre = ab[pl.ds(0, 256), pl.ds(lo + FS, n)]
            sall[pl.ds(0, 256), pl.ds(lo, n)] = (a_pre * jax.nn.sigmoid(a_pre) * b_pre).astype(BF)

        col_tiles(FS, 128, act)
        rs_ready(layer, m)

        def out(lo, n):
            res = mm(sall[pl.ds(0, 256), :], wo[:, pl.ds(lo, n)])
            two[m, :, pl.ds(lo, n)] = res[:128]
            part[:, pl.ds(lo, n)] = res[128:]

        col_tiles(D, 256, out)
        rs_core(layer, m)

    def f3(layer, m):
        tot = rs_total(layer, m)
        h_new = hown[layer, m] + tot.astype(BF)
        hown[layer + 1, m] = h_new
        n_f, inv = norm(h_new)
        ag_sent(layer, m)
        nown[m] = n_f.astype(BF)
        ag_start(layer + 1, layer + 1, m, nown.at[m])

    def b1(layer, m):
        ph = 6 - layer
        cp = ag_load(4 + layer, m, nb, ls.at[5])
        cp.start()
        cp.wait()
        wait_for(ab, ls.at[6])
        rows = pl.ds(pl.multiple_of(m * ROWS, ROWS), ROWS)

        def tile(lo, n):
            t_pre = mm(nb[...], wo[pl.ds(lo, n), :], 1, 1)
            a_pre = ab[:, pl.ds(lo, n)]
            b_pre = ab[:, pl.ds(lo + FS, n)]
            sg = jax.nn.sigmoid(a_pre)
            silu = a_pre * sg
            sall[rows, pl.ds(lo, n)] = (silu * b_pre).astype(BF)
            dab[rows, pl.ds(lo, n)] = (t_pre * b_pre * sg * (1.0 + a_pre * (1.0 - sg))).astype(BF)
            dab[rows, pl.ds(lo + FS, n)] = (t_pre * silu).astype(BF)

        col_tiles(FS, 256, tile)

        @pl.when(m < NM - 1)
        def _():
            pltpu.make_async_copy(AB.at[layer, m + 1], ab, ls.at[6]).start()

        rs_ready(ph, m)
        near = pl.ds(pl.multiple_of(m * ROWS, ROWS), 256)

        def out(lo, n):
            res = mm(dab[near, :], gu[pl.ds(lo, n), :], 1, 1)
            two[m, :, pl.ds(lo, n)] = res[:128]
            part[:, pl.ds(lo, n)] = res[128:]

        @pl.when(m == 0)
        def _():
            wait_for(gu, ls.at[0])

        col_tiles(D, 256, out)
        rs_core(ph, m)

    def b3(layer, m):
        q = rs_total(6 - layer, m)
        n_f, inv = norm(hown[layer, m])
        d_res = inv * (q - n_f * jnp.mean(q * n_f, axis=-1, keepdims=True))
        e_new = (eown[m].astype(F32) + d_res).astype(BF)

        @pl.when(layer < NL - 1)
        def _():
            ag_sent(4 + layer, m)

        eown[m] = e_new

        @pl.when(layer > 0)
        def _():
            ag_start(3 + layer, layer - 1, m, eown.at[m])

        @pl.when(layer == 0)
        def _():
            pltpu.make_async_copy(eown.at[m], dx_ref.at[m, c], ls.at[2]).start()
            rcopy(eown.at[m], dx_ref.at[m, c], dx_s.at[m], dx_r.at[m], (d, 1 - c)).start()
            wait_for(eown.at[m], ls.at[2])

    def grad_cols(layer, which):
        for m in range(NM):
            pltpu.make_async_copy(XALL.at[layer, m, :, pl.ds(pl.multiple_of(which * MS, MS), MS)], gu.at[pl.ds(m * ROWS, ROWS), pl.ds(0, MS)], ls.at[7]).start()
        wait_for(gu.at[:, pl.ds(0, MS)], ls.at[7])

    def w_far(layer):
        p, k = layer // 2, layer % 2
        r, al, be = role(layer)
        an, bn = nbr(layer)
        grad_cols(layer, bn)

        def step(i, carry):
            lo = pl.multiple_of(i * 128, 128)
            wst[...] = mm(gu[:, pl.ds(lo, 128)], dab[...], 0, 0)
            cp = pltpu.make_async_copy(wst, WST.at[layer, pl.ds(lo, 128)], ls.at[8])
            cp.start()
            cp.wait()
            for wi, ref in enumerate((dwg_ref, dwu_ref)):
                dst = ref.at[k, pl.ds(lo, 128), pl.ds(pl.multiple_of(chip(r, c, be) * FS, 128), FS)]
                rcopy(WST.at[layer, pl.ds(lo, 128), pl.ds(wi * FS, FS)], dst, g_bs.at[layer], g_b.at[layer], (bn, p)).start()
            return carry

        lax.fori_loop(0, 4, step, 0)

    def w_near(layer):
        p, k = layer // 2, layer % 2
        r, al, be = role(layer)
        grad_cols(layer, d)

        def step(i, carry):
            lo = pl.multiple_of(i * 128, 128)
            wst[...] = mm(gu[:, pl.ds(lo, 128)], dab[...], 0, 0)

            def dst(ref):
                return ref.at[k, pl.ds(lo, 128), pl.ds(pl.multiple_of(chip(r, c, be) * FS, 128), FS)]

            @pl.when(c == p)
            def _():
                for wi, ref in enumerate((dwg_ref, dwu_ref)):
                    pltpu.make_async_copy(wst.at[:, pl.ds(wi * FS, FS)], dst(ref), ls.at[8]).start()
                wait_for(wst, ls.at[8])

            @pl.when(c != p)
            def _():
                for wi, ref in enumerate((dwg_ref, dwu_ref)):
                    rcopy(wst.at[:, pl.ds(wi * FS, FS)], dst(ref), g_cs.at[layer], g_c.at[layer], (d, p)).start()
                wait_for(wst, g_cs.at[layer])

            return carry

        lax.fori_loop(0, 4, step, 0)

    def w_out(layer):
        p, k = layer // 2, layer % 2
        r, al, be = role(layer)

        @pl.when(c == al)
        def _():
            for m in range(NM):
                pltpu.make_async_copy(XALL.at[4 + layer, m], gu.at[pl.ds(m * ROWS, ROWS), pl.ds(0, D)], ls.at[7]).start()
            wait_for(gu.at[:, pl.ds(0, D)], ls.at[7])

            def step(i, carry):
                lo = pl.multiple_of(i * 128, 128)
                res = wst.at[:, pl.ds(0, D)]
                res[...] = mm(sall[:, pl.ds(lo, 128)], gu[:, pl.ds(0, D)], 0, 0)
                dst = dwo_ref.at[k, pl.ds(lo, 128)]

                @pl.when(c == p)
                def _():
                    cp = pltpu.make_async_copy(res, dst, ls.at[8])
                    cp.start()
                    cp.wait()

                @pl.when(c != p)
                def _():
                    rcopy(res, dst, g_cs.at[layer], g_o.at[layer], (d, p)).start()
                    wait_for(res, g_cs.at[layer])

                return carry

            lax.fori_loop(0, FS // 128, step, 0)

    for m in range(NM):
        pltpu.make_async_copy(x_ref.at[m, c], hown.at[0, m], ls.at[3]).start()
        pltpu.make_async_copy(g_ref.at[m, c], eown.at[m], ls.at[4]).start()
    wait_for(hown.at[0], ls.at[3])
    wait_for(eown, ls.at[4])
    for m in range(NM):
        n_f, inv = norm(hown[0, m])
        nown[m] = n_f.astype(BF)
        ag_start(0, 0, m, nown.at[m])
    w_core(0)
    w_split(0)
    w_pair(0)
    for m in range(NM):
        ag_mid(0, 0, m)
    w_fwd(0)
    w_down(0)
    w_core(1)
    w_split(1)
    w_pair(1)
    w_core(2)
    w_split(2)
    w_core(3)
    for m in range(NM):
        ag_end(0, m)

    def fwd_step(t, carry):
        layer, m = t // NM, t % NM

        @pl.when(m == 0)
        def _():
            w_wait_gu(layer)
            load_gu(layer)

            @pl.when(layer == 1)
            def _():
                w_down(2)
                w_pair(2)
                w_split(3)
                for mm_ in range(NM):
                    ag_start(7, 3, mm_, g_ref.at[mm_, c])

            @pl.when(layer == 2)
            def _():
                w_down(3)
                w_pair(3)
                for mm_ in range(NM):
                    ag_mid(7, 3, mm_)

            wait_for(gu, ls.at[0])

        @pl.when(t > 0)
        def _():
            wait_for(ab, ls.at[6])

        f1(layer, m)

        @pl.when(m == 0)
        def _():
            w_wait_o(layer)
            load_o(layer)
            wait_for(wo, ls.at[1])

        @pl.when(layer < NL - 1)
        def _():
            f1_out(layer, m)

        @pl.when(t == 1)
        def _():
            w_fwd(1)
            w_down(1)

        @pl.when(t == 5)
        def _():
            w_fwd(2)

        @pl.when(t == 9)
        def _():
            w_fwd(3)

        @pl.when(jnp.logical_and(t >= 1, t < 13))
        def _():
            rs_split((t - 1) // NM, (t - 1) // NM, (t - 1) % NM)

        @pl.when(jnp.logical_and(t >= 2, t < 14))
        def _():
            f3((t - 2) // NM, (t - 2) % NM)

        @pl.when(jnp.logical_and(t >= 3, t < 15))
        def _():
            ag_mid((t - 3) // NM + 1, (t - 3) // NM + 1, (t - 3) % NM)
            ag_end((t - 3) // NM + 1, (t - 3) % NM)

        return carry

    lax.fori_loop(0, NL * NM, fwd_step, 0)
    for m in range(NM):
        ag_end(7, m)
    wait_for(ab, ls.at[6])

    def bwd_layer(i, carry):
        layer = NL - 1 - i
        ph = 6 - layer
        pltpu.make_async_copy(AB.at[layer, 0], ab, ls.at[6]).start()

        @pl.when(layer < NL - 1)
        def _():
            load_o(layer)
            load_gu(layer)
            wait_for(wo, ls.at[1])

        @pl.when(layer == NL - 1)
        def _():
            load_gu(layer)

        def gather_mid(m):
            @pl.when(layer > 0)
            def _():
                ag_mid(3 + layer, layer - 1, m)

        def gather_end(m):
            @pl.when(layer > 0)
            def _():
                ag_end(3 + layer, m)

        def step(m, c2):
            b1(layer, m)

            @pl.when(m >= 1)
            def _():
                rs_split(ph, layer, m - 1)

            @pl.when(m >= 2)
            def _():
                b3(layer, m - 2)

            @pl.when(m >= 3)
            def _():
                gather_mid(m - 3)

            return c2

        lax.fori_loop(0, NM, step, 0)
        w_far(layer)
        rs_split(ph, layer, 3)
        b3(layer, 2)
        gather_mid(1)
        gather_end(0)
        w_near(layer)
        b3(layer, 3)
        gather_mid(2)
        gather_end(1)
        w_out(layer)
        gather_mid(3)
        gather_end(2)
        gather_end(3)
        return carry

    lax.fori_loop(0, NL, bwd_layer, 0)

    for m in range(NM):
        wait_for(dx_ref.at[m, 1 - c], dx_r.at[m])
        wait_for(dx_ref.at[m, c], dx_s.at[m])
        ag_sent(3, m)
        ag_sent(7, m)
        wait_for(two.at[m, pl.ds(OWN, OWN)], rb_s.at[6, m])
    wait_for(part, rc_s.at[6, NM - 1])
    for l in range(NL):
        p = l // 2
        r, al, be = role(l)
        wait_for(WGU.at[l, pl.ds(0, MS)], w_s.at[l, 3])

        @pl.when(c == p)
        def _():
            wait_for(WGU.at[l, pl.ds(0, MS)], w_s.at[l, 0])
            wait_for(WGU.at[l, pl.ds(0, 2 * MS)], w_s.at[l, 1])
            wait_for(WGU.at[l, pl.ds(0, 2 * MS)], w_s.at[l, 2])
            wait_for(WO.at[l], w_os.at[l, 1])

            @pl.when(al != p)
            def _():
                wait_for(WO.at[l], w_os.at[l, 0])

        wait_for(WST.at[l], g_bs.at[l])

        @pl.when(c == p)
        def _():
            wait_for(AB.at[0, pl.ds(0, 2)], g_b.at[l])
            wait_for(AB.at[0, 0], g_c.at[l])

            @pl.when(al != p)
            def _():
                wait_for(AB.at[0, pl.ds(0, 2)], g_o.at[l])


def solution(mesh):
    def body(x_loc, g_loc, gate_loc, in_loc, out_loc):
        def hbm(shape, dt):
            return jax.ShapeDtypeStruct(shape, dt)

        any_spec = pl.BlockSpec(memory_space=pl.ANY)
        dma = pltpu.SemaphoreType.DMA
        outs = (
            hbm((NM, 2, OWN, D), BF), hbm((2, MS, 4 * FS), F32), hbm((2, MS, 4 * FS), F32), hbm((2, FS, D), F32),
            hbm((NL, D, F2C), BF), hbm((NL, FS, D), BF), hbm((8, NM, ROWS, D), BF), hbm((NL, NM, ROWS, F2C), F32),
            hbm((7, NM, 128, D), F32), hbm((7, NM, OWN, D), F32), hbm((NL, MS, F2C), F32))
        scratch = [
            pltpu.VMEM((D, F2C), BF), pltpu.VMEM((FS, D), BF), pltpu.VMEM((ROWS, D), BF), pltpu.VMEM((ROWS, F2C), F32),
            pltpu.VMEM((NM * ROWS, F2C), BF), pltpu.VMEM((NM * ROWS, FS), BF), pltpu.VMEM((128, D), F32),
            pltpu.VMEM((NM, 128, D), F32), pltpu.VMEM((128, D), F32), pltpu.VMEM((OWN, D), F32),
            pltpu.VMEM((NL, NM, OWN, D), BF), pltpu.VMEM((NM, OWN, D), BF), pltpu.VMEM((NM, OWN, D), BF), pltpu.VMEM((128, F2C), F32),
            dma((9,)), dma((NL,)), dma((NL, 2, 2)), dma((NL,)), dma((NL,)), dma((NL,)), dma((NL, 4)), dma((NL, 2)),
            dma((8, NM)), dma((8, NM)), dma((8, NM)), dma((8, NM)), dma((8, NM)),
            dma((7, NM)), dma((7, NM)), dma((7, NM)), dma((7, NM)), dma((NL,)), dma((NL,)), dma((NL,)), dma((NL,)), dma((NL,)),
            dma((NM,)), dma((NM,))]
        res = pl.pallas_call(
            kernel, out_shape=outs, in_specs=[any_spec] * 5, out_specs=(any_spec,) * len(outs), scratch_shapes=scratch,
            compiler_params=pltpu.CompilerParams(collective_id=0, has_side_effects=True, vmem_limit_bytes=67043328),
        )(x_loc.reshape(NM, 2, OWN, D), g_loc.reshape(NM, 2, OWN, D), gate_loc[0], in_loc[0], out_loc[0])
        return res[0].reshape(x_loc.shape), res[1][None], res[2][None], res[3][None]

    act_spec = P(None, "data", None, None)
    weight_spec = P("stage", None, "data", None)
    return jax.shard_map(body, mesh=mesh, in_specs=(act_spec, act_spec, weight_spec, weight_spec, weight_spec), out_specs=(act_spec, weight_spec, weight_spec, weight_spec), check_vma=False)
```

```python
import jax
import jax.numpy as jnp
from jax import lax
from jax.experimental import pallas as pl
from jax.experimental.pallas import tpu as pltpu
from jax.sharding import PartitionSpec as P

EPS = 1e-6
BF = jnp.bfloat16
F32 = jnp.float32
MESH = pl.DeviceIdType.MESH

NL = 4
NM = 4
OWN = 64
ROWS = 512
D = 2048
FS = 1408
F2C = 2 * FS
SPLIT = 768
ONE, TWO = 1, 2
LAST = NL - ONE
HALF = 256
QUART = 128
FAR = 4
NP = 8
NS = 7
CORES = range(TWO)
MS = 512


(S_GU, S_O, S_OWN, S_TC, S_TB, S_NEAR, S_AB, S_COL, S_ST, S_ST1, S_AB1, S_FAR, S_SX, S_H, S_H1, S_H2, S_H3, S_HL) = range(18)


def mm(lhs, rhs, ld=1, rd=0):
    return lax.dot_general(lhs, rhs, (((ld,), (rd,)), ((), ())), preferred_element_type=F32)


def col_tiles(total, tile, body):
    full = total // tile

    def step(idx, carry):
        body(pl.multiple_of(idx * tile, tile), tile)
        return carry

    lax.fori_loop(0, full, step, 0)
    if total % tile:
        body(full * tile, total % tile)


def flip(v):
    return ONE - v


def home(layer):
    return layer // TWO, layer % TWO


def kernel(x_ref, g_ref, wg_ref, wu_ref, wo_ref,
           dx_ref, dwg_ref, dwu_ref, dwo_ref, WSP, WOS, WGU, WO, XALL, AB, RC, RB, WST, SX, H,
           gu, wo, nb, ab, dab, sall, part, two, tc, tb, hown, eown, nown, wst, ncol,
           ls, w_spr, w_osr, w_t2r, w_br, w_ar, w_abr, w_or, w_s, w_os, ag_b, ag_a, ag_d, ag_c0, ag_c1, ag_s,
           rc_r, rc_s, rb_r, rb_s, g_b, g_c, g_o, g_bs, sx_r, sx_s, dx_r, dx_s):
    d = lax.axis_index("data")
    c = lax.axis_index("stage")
    y, x = home(d)
    mate = (d, 1 - c)

    def role(layer):
        p, r = home(layer)
        al = x + r * (y - x)
        be = y + r * (x - y)
        return r, al, be

    def chip(r, al, be):
        return be * (2 - r) + al * (1 + r)

    def nbr(layer):
        r, al, be = role(layer)
        return chip(r, flip(al), be), chip(r, al, flip(be))

    def rcopy(src, dst, ssem, rsem, dev):
        return pltpu.make_async_remote_copy(src_ref=src, dst_ref=dst, send_sem=ssem, recv_sem=rsem, device_id=dev, device_id_type=MESH)

    def wait_for(region, sem):
        pltpu.make_async_copy(region, region, sem).wait()

    bar = pltpu.get_barrier_semaphore()
    for dd in range(1, 4):
        for cc in CORES:
            pl.semaphore_signal(bar, inc=1, device_id=((d + dd) % 4, cc), device_id_type=MESH)
    pl.semaphore_signal(bar, inc=1, device_id=mate, device_id_type=MESH)
    pl.semaphore_wait(bar, 7)

    def blk(ref, k, fs, lo, n):
        return ref.at[k, pl.ds(lo, n), pl.ds(pl.multiple_of(fs * FS, QUART), FS)]

    def w_dst(l, row, wi, n):
        return WGU.at[l, pl.ds(row, n), pl.ds(wi * FS, FS)]

    def w_core(l):
        p, k = home(l)
        r, al, be = role(l)
        row = pl.multiple_of(d * MS, MS)

        @pl.when(c == p)
        def _():
            for wi, ref in enumerate((wg_ref, wu_ref)):
                rcopy(blk(ref, k, chip(r, 1 - p, flip(be)), 0, MS), WSP.at[l, :, pl.ds(wi * FS, FS)], w_s.at[l, 0], w_spr.at[l], mate).start()
                rcopy(blk(ref, k, chip(r, 1 - p, be), 0, MS), w_dst(l, row, wi, MS), w_s.at[l, 0], w_t2r.at[l], mate).start()

    def w_core_o(l):
        p, k = home(l)
        r, al, be = role(l)

        @pl.when(c == p)
        def _():
            rcopy(wo_ref.at[k, pl.ds(FS // 2, FS // 2)], WOS.at[l], w_os.at[l, 2], w_osr.at[l], mate).start()

            @pl.when(al != p)
            def _():
                rcopy(wo_ref.at[k], WO.at[l], w_os.at[l, 0], w_or.at[l], (d, al)).start()

    def w_split(l, pieces=(0, 1, 2, 3)):
        p, k = home(l)
        r, al, be = role(l)
        row = pl.multiple_of(d * MS, MS)
        bn = chip(r, al, flip(be))

        def go(get):
            for half, wi in [home(q) for q in pieces]:
                rcopy(get(wi, half * HALF), w_dst(l, row + half * HALF, wi, HALF), w_s.at[l, 1], w_br.at[l, wi, half], (bn, c)).start()

        @pl.when(c == p)
        def _():
            go(lambda wi, lo: blk((wg_ref, wu_ref)[wi], k, chip(r, c, flip(be)), lo, HALF))

        @pl.when(c != p)
        def _():
            if 0 in pieces:
                wait_for(WSP.at[l], w_spr.at[l])
            go(lambda wi, lo: WSP.at[l, pl.ds(lo, HALF), pl.ds(wi * FS, FS)])

    def w_pair(l, pieces=(0, 1, 2, 3)):
        p, k = home(l)
        r, al, be = role(l)
        row = pl.multiple_of(d * MS, MS)
        an = chip(r, flip(al), be)

        def go(get):
            for half, wi in [home(q) for q in pieces]:
                rcopy(get(wi, half * HALF), w_dst(l, row + half * HALF, wi, HALF), w_s.at[l, 2], w_ar.at[l], (an, c)).start()

        @pl.when(c == p)
        def _():
            go(lambda wi, lo: blk((wg_ref, wu_ref)[wi], k, chip(r, c, be), lo, HALF))

        @pl.when(c != p)
        def _():
            if 0 in pieces:
                wait_for(WGU.at[l, pl.ds(row, MS)], w_t2r.at[l])
            go(lambda wi, lo: w_dst(l, row + lo, wi, HALF))

    def w_fwd(l, pieces=(0, 1, 2, 3)):
        r, al, be = role(l)
        an, bn = nbr(l)
        row = pl.multiple_of(bn * MS, MS)
        for half, wi in [home(q) for q in pieces]:
            src = w_dst(l, row + half * HALF, wi, HALF)
            wait_for(src, w_br.at[l, wi, half])
            rcopy(src, src, w_s.at[l, 3], w_abr.at[l], (an, c)).start()

    def w_down(l, pieces=(0, 1, 2, 3)):
        p, k = home(l)
        r, al, be = role(l)
        an = chip(r, flip(al), be)
        half, n = FS // 2, FS // 8

        @pl.when(c == p)
        def _():
            for q in pieces:
                rcopy(wo_ref.at[k, pl.ds(q * n, n)], WO.at[l, pl.ds(q * n, n)], w_os.at[l, 1], w_or.at[l], (an, al)).start()

        @pl.when(c != p)
        def _():
            if 0 in pieces:
                wait_for(WOS.at[l], w_osr.at[l])
            for q in pieces:
                rcopy(WOS.at[l, pl.ds(q * n, n)], WO.at[l, pl.ds(half + q * n, n)], w_os.at[l, 1], w_or.at[l], (an, al)).start()

    def w_wait_gu(l):
        r, al, be = role(l)
        an, bn = nbr(l)
        abn = chip(r, flip(al), flip(be))

        wait_for(WGU.at[l, pl.ds(pl.multiple_of(an * MS, MS), MS)], w_ar.at[l])
        wait_for(WGU.at[l, pl.ds(pl.multiple_of(abn * MS, MS), MS)], w_abr.at[l])

    def w_wait_o(l):
        p, k = home(l)
        r, al, be = role(l)

        @pl.when(jnp.logical_not(jnp.logical_and(c == al, c == p)))
        def _():
            wait_for(WO.at[l], w_or.at[l])

    def load_gu(l):
        p, k = home(l)
        r, al, be = role(l)
        for dd in range(1, 4):
            row = pl.multiple_of(((d + dd) % 4) * MS, MS)
            pltpu.make_async_copy(WGU.at[l, pl.ds(row, MS)], gu.at[pl.ds(row, MS)], ls.at[S_GU]).start()
        row = pl.multiple_of(d * MS, MS)

        @pl.when(c == p)
        def _():
            for wi, ref in enumerate((wg_ref, wu_ref)):
                pltpu.make_async_copy(blk(ref, k, chip(r, c, be), 0, MS), gu.at[pl.ds(row, MS), pl.ds(wi * FS, FS)], ls.at[S_GU]).start()

        @pl.when(c != p)
        def _():
            pltpu.make_async_copy(WGU.at[l, pl.ds(row, MS)], gu.at[pl.ds(row, MS)], ls.at[S_GU]).start()

    def load_o(l):
        p, k = home(l)
        r, al, be = role(l)
        mine = jnp.logical_and(c == al, c == p)

        @pl.when(mine)
        def _():
            pltpu.make_async_copy(wo_ref.at[k], wo, ls.at[S_O]).start()

        @pl.when(jnp.logical_not(mine))
        def _():
            pltpu.make_async_copy(WO.at[l], wo, ls.at[S_O]).start()

    def slot(ph, m, lo, n):
        return XALL.at[ph, m, pl.ds(lo * OWN, n * OWN)]

    def ag_start(ph, layer, m, src):
        an, bn = nbr(layer)
        pltpu.make_async_copy(src, slot(ph, m, 0, 1), ls.at[S_OWN]).start()
        rcopy(src, slot(ph, m, ONE, ONE), ag_s.at[ph, m], ag_b.at[ph, m], (bn, c)).start()
        rcopy(src, slot(ph, m, FAR, ONE), ag_s.at[ph, m], ag_a.at[ph, m], (an, c)).start()
        wait_for(slot(ph, m, 0, 1), ls.at[S_OWN])

    def other_way(ph):
        return jnp.logical_and(ph != 1, jnp.logical_or(ph < NL, ph >= NP - TWO))

    def ag_mid(ph, layer, m):
        an, bn = nbr(layer)
        alt = other_way(ph)
        wait_for(slot(ph, m, ONE, ONE), ag_b.at[ph, m])
        rcopy(slot(ph, m, 0, TWO), slot(ph, m, TWO, TWO), ag_s.at[ph, m], ag_c0.at[ph, m], mate).start()

        @pl.when(jnp.logical_not(alt))
        def _():
            rcopy(slot(ph, m, ONE, ONE), slot(ph, m, FAR + ONE, ONE), ag_s.at[ph, m], ag_d.at[ph, m], (an, c)).start()

        @pl.when(alt)
        def _():
            wait_for(slot(ph, m, FAR, ONE), ag_a.at[ph, m])
            rcopy(slot(ph, m, FAR, ONE), slot(ph, m, FAR + ONE, ONE), ag_s.at[ph, m], ag_d.at[ph, m], (bn, c)).start()

    def ag_end(ph, m):
        @pl.when(jnp.logical_not(other_way(ph)))
        def _():
            wait_for(slot(ph, m, FAR, ONE), ag_a.at[ph, m])

        wait_for(slot(ph, m, FAR + ONE, ONE), ag_d.at[ph, m])
        rcopy(slot(ph, m, FAR, TWO), slot(ph, m, FAR + TWO, TWO), ag_s.at[ph, m], ag_c1.at[ph, m], mate).start()

    def ag_load(ph, m, half):
        wait_for(slot(ph, m, 2 + 4 * half, 2), (ag_c0, ag_c1)[half].at[ph, m])
        rows = pl.ds(half * HALF, HALF)
        pltpu.make_async_copy(XALL.at[ph, m, rows], nb.at[rows], ls.at[(S_NEAR, S_FAR)[half]]).start()

    def ag_loaded(half):
        wait_for(nb.at[pl.ds(half * HALF, HALF)], ls.at[(S_NEAR, S_FAR)[half]])

    def ag_sent(ph, m):
        wait_for(slot(ph, m, 0, 7), ag_s.at[ph, m])

    def norm(h_rows):
        h_f = h_rows.astype(F32)
        inv = lax.rsqrt(jnp.mean(h_f * h_f, axis=-1, keepdims=True) + EPS)
        return h_f * inv, inv

    def rs_core(ph, m):
        rcopy(part, RC.at[ph, m], rc_s.at[ph, m], rc_r.at[ph, m], mate).start()

    def rs_load(ph, m):
        wait_for(RC.at[ph, m], rc_r.at[ph, m])
        pltpu.make_async_copy(RC.at[ph, m], tc, ls.at[S_TC]).start()

    def rs_split(ph, layer, m):
        an, bn = nbr(layer)
        wait_for(tc, ls.at[S_TC])
        two[m] = two[m] + tc[...]
        rcopy(two.at[m, pl.ds(OWN, OWN)], RB.at[ph, m], rb_s.at[ph, m], rb_r.at[ph, m], (bn, c)).start()

    def rs_total_load(ph, m):
        wait_for(RB.at[ph, m], rb_r.at[ph, m])
        pltpu.make_async_copy(RB.at[ph, m], tb, ls.at[S_TB]).start()

    def rs_total(ph, m):
        wait_for(tb, ls.at[S_TB])
        return two[m, pl.ds(0, OWN)] + tb[...]

    def rs_ready(ph, m):
        first = jnp.logical_and(ph == 0, m == 0)
        pph = jnp.where(m == 0, ph - 1, ph)
        pm = jnp.where(m == 0, NM - 1, m - 1)

        @pl.when(jnp.logical_not(first))
        def _():
            wait_for(part, rc_s.at[pph, pm])

        @pl.when(ph > 0)
        def _():
            wait_for(two.at[m, pl.ds(OWN, OWN)], rb_s.at[ph - 1, m])

    def pre(layer, m, half):
        rows = pl.ds(half * HALF, HALF)
        ab[rows, :] = mm(nb[rows, :], gu[...])

        @pl.when(layer < LAST)
        def _():
            pltpu.make_async_copy(ab.at[rows], AB.at[layer, m, rows], ls.at[S_AB + 4 * half]).start()

    def ab_wait(half):
        wait_for(ab.at[pl.ds(half * HALF, HALF)], ls.at[S_AB + 4 * half])

    def f1_out(layer, m):
        def act(lo, n):
            a_pre = ab[pl.ds(0, HALF), pl.ds(lo, n)]
            b_pre = ab[pl.ds(0, HALF), pl.ds(lo + FS, n)]
            sall[pl.ds(0, HALF), pl.ds(lo, n)] = (a_pre * jax.nn.sigmoid(a_pre) * b_pre).astype(BF)

        col_tiles(FS, 128, act)
        rs_ready(layer, m)

        def out(lo, n):
            res = mm(sall[pl.ds(0, HALF), :], wo[:, pl.ds(lo, n)])
            two[m, :, pl.ds(lo, n)] = res[:128]
            part[:, pl.ds(lo, n)] = res[128:]

        col_tiles(D, 1024, out)
        rs_core(layer, m)

    def f3(layer, m):
        rs_total_load(layer, m)
        tot = rs_total(layer, m)
        h_new = hown[m] + tot.astype(BF)

        @pl.when(layer > 0)
        def _():
            wait_for(hown.at[m], ls.at[S_H + m])

        hown[m] = h_new

        @pl.when(layer < NL - 2)
        def _():
            pltpu.make_async_copy(hown.at[m], H.at[layer, m], ls.at[S_H + m]).start()

        n_f, inv = norm(h_new)
        ag_sent(layer, m)
        nown[m] = n_f.astype(BF)
        ag_start(layer + 1, layer + 1, m, nown.at[m])

    def b1(layer, m, half, loaded=False, between=None):
        rows = pl.ds(half * HALF, HALF)
        ag_loaded(half)
        t_buf = wst.at[half, :, pl.ds(0, FS)]
        t_buf[...] = mm(nb[rows, :], wo[...], ONE, ONE)
        if not loaded:
            ab_wait(half)
        if between is not None:
            between()
        into = pl.ds(pl.multiple_of(m * ROWS + half * HALF, HALF), 256)

        def tile(lo, n):
            t_pre = t_buf[:, pl.ds(lo, n)]
            a_pre = ab[rows, pl.ds(lo, n)]
            b_pre = ab[rows, pl.ds(lo + FS, n)]
            sg = jax.nn.sigmoid(a_pre)
            silu = a_pre * sg
            sall[into, pl.ds(lo, n)] = (silu * b_pre).astype(BF)
            dab[into, pl.ds(lo, n)] = (t_pre * b_pre * sg * (1.0 + a_pre * (1.0 - sg))).astype(BF)
            dab[into, pl.ds(lo + FS, n)] = (t_pre * silu).astype(BF)

        col_tiles(FS, 128, tile)
        r, al, be = role(layer)

        @pl.when(c == al)
        def _():
            for near in CORES:
                src = pl.ds(pl.multiple_of(m * ROWS + half * HALF + near * 128, 128), QUART)
                dst = pl.ds(pl.multiple_of(m * ROWS + half * HALF + (1 - near) * 128, 128), QUART)
                rcopy(sall.at[src, pl.ds(SPLIT, FS - SPLIT)], SX.at[layer, dst], sx_s.at[layer], sx_r.at[layer], mate).start()

        if not loaded:
            @pl.when(m < NM - 1)
            def _():
                pltpu.make_async_copy(AB.at[layer, m + 1, rows], ab.at[rows], ls.at[S_AB + 4 * half]).start()

    def b1_out(layer, m):
        ph = NS - ONE - layer
        rs_ready(ph, m)
        near = pl.ds(pl.multiple_of(m * ROWS, ROWS), 256)

        @pl.when(jnp.logical_and(m == 0, layer < LAST))
        def _():
            wait_for(gu, ls.at[S_GU])

        def out(lo, n):
            res = mm(dab[near, :], gu[pl.ds(lo, n), :], ONE, ONE)
            two[m, :, pl.ds(lo, n)] = res[:128]
            part[:, pl.ds(lo, n)] = res[128:]

        col_tiles(D, 1024, out)
        rs_core(ph, m)

    def b3(layer, m):
        q = rs_total(NS - ONE - layer, m)
        n_f, inv = norm(hown[m])
        d_res = inv * (q - n_f * jnp.mean(q * n_f, axis=-1, keepdims=True))
        e_new = (eown[m].astype(F32) + d_res).astype(BF)

        ag_sent(NL + layer, m)
        eown[m] = e_new

        @pl.when(layer > 0)
        def _():
            ag_start(NL - ONE + layer, layer - 1, m, eown.at[m])

        @pl.when(layer == 0)
        def _():
            pltpu.make_async_copy(eown.at[m], dx_ref.at[m, c], ls.at[S_OWN]).start()
            rcopy(eown.at[m], dx_ref.at[m, c], dx_s.at[m], dx_r.at[m], mate).start()
            wait_for(eown.at[m], ls.at[S_OWN])

    def grad_cols(layer, which):
        for m in range(NM):
            pltpu.make_async_copy(XALL.at[layer, m, :, pl.ds(pl.multiple_of(which * MS, MS), MS)], ncol.at[pl.ds(m * ROWS, ROWS)], ls.at[S_COL]).start()

    def w_far(layer, i):
        wst[i] = mm(ncol[:, pl.ds(i * HALF, HALF)], dab[...], 0, 0)
        pltpu.make_async_copy(wst.at[i], WST.at[layer, pl.ds(i * HALF, HALF)], ls.at[S_ST + i]).start()

    def w_send(layer, piece):
        p, k = home(layer)
        r, al, be = role(layer)
        an, bn = nbr(layer)
        rows = pl.ds(pl.multiple_of((piece // 2) * 64, 64), 64)
        for wi, ref in enumerate((dwg_ref, dwu_ref)):
            @pl.when(piece % 2 == wi)
            def _():
                dst = ref.at[k, rows, pl.ds(pl.multiple_of(chip(r, c, be) * FS, QUART), FS)]
                rcopy(WST.at[layer, rows, pl.ds(wi * FS, FS)], dst, g_bs.at[layer], g_b.at[layer], (bn, p)).start()

    def w_sends(layer, lo, n):
        def step(i, carry):
            w_send(layer, i)
            return carry

        lax.fori_loop(lo, lo + n, step, 0)

    def out_load(layer):
        r, al, be = role(layer)
        for m in range(NM):
            pltpu.make_async_copy(XALL.at[NL + layer, m], gu.at[pl.ds(m * ROWS, ROWS), pl.ds(0, D)], ls.at[S_GU]).start()

        @pl.when(c != al)
        def _():
            wait_for(SX.at[layer], sx_r.at[layer])
            pltpu.make_async_copy(SX.at[layer], sall.at[:, pl.ds(SPLIT, FS - SPLIT)], ls.at[S_SX]).start()

    def w_near(layer, i):
        p, k = home(layer)
        r, al, be = role(layer)
        wst[i] = mm(ncol[:, pl.ds(i * HALF, HALF)], dab[...], 0, 0)
        for wi, ref in enumerate((dwg_ref, dwu_ref)):
            src = wst.at[i, :, pl.ds(wi * FS, FS)]
            dst = ref.at[k, pl.ds(i * HALF, HALF), pl.ds(pl.multiple_of(chip(r, c, be) * FS, QUART), FS)]

            @pl.when(c == p)
            def _():
                pltpu.make_async_copy(src, dst, ls.at[S_ST + i]).start()

            @pl.when(c != p)
            def _():
                rcopy(src, dst, ls.at[S_ST + i], g_c.at[layer], (d, p)).start()

    def near_end():
        for i in CORES:
            wait_for(wst.at[i], ls.at[S_ST + i])

    def w_out(layer, tiles):
        p, k = home(layer)
        r, al, be = role(layer)
        base = jnp.where(c == al, 0, SPLIT)

        def rows_of(slot, n):
            return wst.at[slot, pl.ds(0, n), pl.ds(0, D)]

        def one(i, slot, n):
            lo = pl.multiple_of(base + i * HALF, 128)
            res = rows_of(slot, n)
            res[...] = mm(sall[:, pl.ds(lo, n)], gu[:, pl.ds(0, D)], 0, 0)
            dst = dwo_ref.at[k, pl.ds(lo, n)]

            @pl.when(c == p)
            def _():
                pltpu.make_async_copy(res, dst, ls.at[S_ST + slot]).start()

            @pl.when(c != p)
            def _():
                rcopy(res, dst, ls.at[S_ST + slot], g_o.at[layer], (d, p)).start()

        if 0 in tiles:
            wait_for(gu.at[:, pl.ds(0, D)], ls.at[S_GU])

            @pl.when(c != al)
            def _():
                wait_for(SX.at[layer], ls.at[S_SX])

            def step(i, carry):
                one(i, i, 256)
                return carry

            lax.fori_loop(0, 2, step, 0)
        if 2 in tiles:
            wait_for(rows_of(0, 256), ls.at[S_ST])

            @pl.when(c == al)
            def _():
                one(2, 0, 256)
                wait_for(rows_of(0, 256), ls.at[S_ST])
                wait_for(SX.at[layer], sx_s.at[layer])

            @pl.when(c != al)
            def _():
                one(2, 0, 128)
                wait_for(rows_of(0, 128), ls.at[S_ST])

            wait_for(rows_of(1, 256), ls.at[S_ST1])

    w_core(0)
    for m in range(NM):
        pltpu.make_async_copy(x_ref.at[m, c], hown.at[m], ls.at[S_TC]).start()
        pltpu.make_async_copy(g_ref.at[m, c], eown.at[m], ls.at[S_TB]).start()
    w_split(0)
    w_pair(0)
    w_core_o(0)
    wait_for(hown, ls.at[S_TC])
    wait_for(eown, ls.at[S_TB])
    for m in range(NM):
        n_f, inv = norm(hown[m])
        nown[m] = n_f.astype(BF)
        ag_start(0, 0, m, nown.at[m])
    for l in range(1, NL):
        w_core(l)
        w_core_o(l)
    w_pair(1)
    w_fwd(0)
    for m in range(NM):
        ag_mid(0, 0, m)
    w_down(0)
    w_split(1)
    w_down(1)

    def fwd_step(t, carry):
        layer, m = t // NM, t % NM

        @pl.when(m == 0)
        def _():
            w_wait_gu(layer)
            load_gu(layer)
            wait_for(gu, ls.at[S_GU])

        @pl.when(jnp.logical_and(t > 0, t < 13))
        def _():
            ab_wait(0)

        @pl.when(t <= 12)
        def _():
            ag_load(layer, m, 0)

        ag_loaded(0)
        pre(layer, m, 0)

        @pl.when(m == 0)
        def _():
            w_wait_o(layer)
            load_o(layer)
            wait_for(wo, ls.at[S_O])

        @pl.when(layer < LAST)
        def _():
            f1_out(layer, m)

        @pl.when(layer == LAST)
        def _():
            ag_load(NL + layer, m, 0)

        @pl.when(jnp.logical_and(t >= 2, t < 14))
        def _():
            f3((t - 2) // NM, (t - 2) % NM)

        @pl.when(jnp.logical_and(t >= 3, t < 15))
        def _():
            ag_mid((t - 3) // NM + 1, (t - 3) // NM + 1, (t - 3) % NM)

        ag_end(layer, m)

        @pl.when(jnp.logical_and(t > 0, t < 13))
        def _():
            ab_wait(1)

        ag_load(layer, m, 1)

        @pl.when(layer == LAST)
        def _():
            b1(layer, m, 0, True)
            b1_out(layer, m)

            @pl.when(m < NM - 1)
            def _():
                ag_load(layer, m + 1, 0)

        ag_loaded(1)
        pre(layer, m, 1)

        @pl.when(layer < LAST)
        def _():
            rs_load(layer, m)
            rs_split(layer, layer, m)

        @pl.when(layer == LAST)
        def _():
            ag_load(NL + layer, m, 1)

            @pl.when(m >= 2)
            def _():
                rs_total_load(NS - ONE - layer, m - 2)
                b3(layer, m - 2)

            b1(layer, m, 1, True, lambda: rs_load(NS - ONE - layer, m))
            rs_split(NS - ONE - layer, layer, m)

        def at(step, *work):
            @pl.when(t == step)
            def _():
                for fn in work:
                    fn()

        def each(fn):
            for m_ in range(NM):
                fn(NP - ONE, LAST, m_)

        plan = ("F1a P2a", "F1bc P2b", "F1d S2a P2c", "S2bcd P2d", "P3ab F2a", "F2bcd P3cd D2a",
                "D2bcd D3ab", "S3abcd D3cd", "", "F3a", "F3b", "F3cd")
        sends = {"F": w_fwd, "P": w_pair, "S": w_split, "D": w_down}
        for step, words in enumerate(plan):
            for w in words.split():
                at(step, lambda: sends[w[:ONE]](int(w[ONE:TWO]), ["abcd".index(q) for q in w[TWO:]]))

        at(7, lambda: each(lambda ph, l, m_: ag_start(ph, l, m_, eown.at[m_])))
        at(9, lambda: each(ag_mid))
        at(11, lambda: each(lambda ph, l, m_: ag_end(ph, m_)))
        return carry

    lax.fori_loop(0, NL * NM, fwd_step, 0)

    def bwd_layer(i, carry):
        layer = LAST - i
        ph = NS - ONE - layer
        an, bn = nbr(layer)
        grad_cols(layer, bn)

        @pl.when(layer < LAST)
        def _():
            for half in CORES:
                rows = pl.ds(half * HALF, HALF)
                pltpu.make_async_copy(AB.at[layer, 0, rows], ab.at[rows], ls.at[S_AB + 4 * half]).start()
            load_o(layer)
            load_gu(layer)

            @pl.when(layer > 0)
            def _():
                pltpu.make_async_copy(H.at[layer - 1], hown, ls.at[S_HL]).start()

            @pl.when(layer == 0)
            def _():
                for m in range(NM):
                    pltpu.make_async_copy(x_ref.at[m, c], hown.at[m], ls.at[S_HL]).start()

            wait_for(wo, ls.at[S_O])
            wait_for(hown, ls.at[S_HL])

        def gather_mid(m):
            @pl.when(layer > 0)
            def _():
                ag_mid(NL - ONE + layer, layer - 1, m)

        def bulk(lyr, at, n, *only):
            for v in only:
                @pl.when(layer == v)
                def _():
                    w_sends(lyr, at, n)

        bulk(3, 4, 1, 2)
        bulk(3, 13, 3, 1)
        bulk(2, 0, 1, 1)
        bulk(2, 11, 5, 0)
        bulk(1, 0, 4, 0)

        def step(m, c2):
            ag_load(NL + layer, m, 1)
            b1(layer, m, 0)

            @pl.when(m >= 2)
            def _():
                rs_total_load(ph, m - 2)

            b1_out(layer, m)

            @pl.when(m < NM - 1)
            def _():
                ag_end(NL + layer, m + 1)
                ag_load(NL + layer, m + 1, 0)

            @pl.when(m >= 2)
            def _():
                b3(layer, m - 2)

            bulk(3, 5 + 2 * m, 1, 2)
            bulk(2, 1 + 2 * m, 1, 1)
            b1(layer, m, 1, False, lambda: rs_load(ph, m))
            rs_split(ph, layer, m)
            bulk(3, 6 + 2 * m, 1, 2)
            bulk(2, 2 + 2 * m, 1, 1)
            bulk(1, 4 + 3 * m, 3, 0)
            return c2

        @pl.when(layer < LAST)
        def _():
            ag_load(NL + layer, 0, 0)
            lax.fori_loop(0, NM, step, 0)

        out_load(layer)
        wait_for(ncol, ls.at[S_COL])
        w_far(layer, 0)
        rs_total_load(ph, 2)
        w_far(layer, 1)
        b3(layer, 2)
        grad_cols(layer, d)
        near_end()

        @pl.when(layer == 0)
        def _():
            w_sends(0, 0, 16)

        gather_mid(0)
        wait_for(ncol, ls.at[S_COL])
        w_near(layer, 0)
        rs_total_load(ph, 3)
        b3(layer, 3)
        bulk(3, 0, 1, 3)
        w_near(layer, 1)
        bulk(3, 1, 1, 3)
        gather_mid(1)
        near_end()
        w_out(layer, (0, 1))
        bulk(3, 2, 1, 3)
        bulk(2, 9, 1, 1)
        gather_mid(2)
        w_out(layer, (2,))
        bulk(3, 3, 1, 3)
        bulk(2, 10, 1, 1)
        gather_mid(3)

        @pl.when(layer > 0)
        def _():
            ag_end(NL - ONE + layer, 0)

        return carry

    lax.fori_loop(0, NL, bwd_layer, 0)

    for m in range(NM):
        wait_for(dx_ref.at[m, 1 - c], dx_r.at[m])
        wait_for(dx_ref.at[m, c], dx_s.at[m])
        ag_sent(3, m)
        wait_for(two.at[m, pl.ds(OWN, OWN)], rb_s.at[6, m])
    wait_for(part, rc_s.at[6, NM - 1])
    for l in range(NL):
        p, k = home(l)
        r, al, be = role(l)
        for i in range(1, 4):
            wait_for(WGU.at[l, pl.ds(0, MS)], w_s.at[l, i])
        wait_for(WOS.at[l], w_os.at[l, 1])

        @pl.when(c == p)
        def _():
            wait_for(WGU.at[l, pl.ds(0, 2 * MS)], w_s.at[l, 0])
            wait_for(WOS.at[l], w_os.at[l, 2])

            @pl.when(al != p)
            def _():
                wait_for(WO.at[l], w_os.at[l, 0])

        wait_for(WST.at[l], g_bs.at[l])

        @pl.when(c == p)
        def _():
            wait_for(AB.at[0, pl.ds(0, 2)], g_b.at[l])
            wait_for(AB.at[0, 0], g_c.at[l])

            @pl.when(al != p)
            def _():
                wait_for(dwo_ref.at[0, pl.ds(0, SPLIT)], g_o.at[l])

            @pl.when(al == p)
            def _():
                wait_for(dwo_ref.at[0, pl.ds(0, FS - SPLIT)], g_o.at[l])


def solution(mesh):
    def body(x_loc, g_loc, gate_loc, in_loc, out_loc):
        def hbm(shape, dt):
            return jax.ShapeDtypeStruct(shape, dt)

        any_spec = pl.BlockSpec(memory_space=pl.ANY)
        dma = pltpu.SemaphoreType.DMA
        outs = (
            hbm((NM, 2, OWN, D), BF), hbm((2, MS, 4 * FS), F32), hbm((2, MS, 4 * FS), F32), hbm((2, FS, D), F32),
            hbm((NL, MS, F2C), BF), hbm((NL, FS // 2, D), BF),
            hbm((NL, D, F2C), BF), hbm((NL, FS, D), BF), hbm((NP, NM, ROWS, D), BF), hbm((NL, NM, ROWS, F2C), F32),
            hbm((NS, NM, QUART, D), F32), hbm((NS, NM, OWN, D), F32), hbm((NL, MS, F2C), F32), hbm((NL, NM * ROWS, FS - SPLIT), BF), hbm((2, NM, OWN, D), BF))
        scratch = [
            pltpu.VMEM((D, F2C), BF), pltpu.VMEM((FS, D), BF), pltpu.VMEM((ROWS, D), BF), pltpu.VMEM((ROWS, F2C), F32),
            pltpu.VMEM((NM * ROWS, F2C), BF), pltpu.VMEM((NM * ROWS, FS), BF), pltpu.VMEM((QUART, D), F32),
            pltpu.VMEM((NM, QUART, D), F32), pltpu.VMEM((QUART, D), F32), pltpu.VMEM((OWN, D), F32),
            pltpu.VMEM((NM, OWN, D), BF), pltpu.VMEM((NM, OWN, D), BF), pltpu.VMEM((NM, OWN, D), BF), pltpu.VMEM((2, 256, F2C), F32), pltpu.VMEM((NM * ROWS, MS), BF),
            dma((S_HL + ONE,)), dma((NL,)), dma((NL,)), dma((NL,)), dma((NL, 2, 2)), dma((NL,)), dma((NL,)), dma((NL,)), dma((NL, 4)), dma((NL, 3)),
            dma((NP, NM)), dma((NP, NM)), dma((NP, NM)), dma((NP, NM)), dma((NP, NM)), dma((NP, NM)),
            dma((NS, NM)), dma((NS, NM)), dma((NS, NM)), dma((NS, NM)), dma((NL,)), dma((NL,)), dma((NL,)), dma((NL,)), dma((NL,)), dma((NL,)),
            dma((NM,)), dma((NM,))]
        res = pl.pallas_call(
            kernel, out_shape=outs, in_specs=[any_spec] * 5, out_specs=(any_spec,) * len(outs), scratch_shapes=scratch,
            compiler_params=pltpu.CompilerParams(collective_id=0, has_side_effects=True, vmem_limit_bytes=67043328),
        )(x_loc.reshape(NM, 2, OWN, D), g_loc.reshape(NM, 2, OWN, D), gate_loc[0], in_loc[0], out_loc[0])
        return res[0].reshape(x_loc.shape), res[1][None], res[2][None], res[3][None]

    act_spec = P(None, "data", None, None)
    weight_spec = P("stage", None, "data", None)
    return jax.shard_map(body, mesh=mesh, in_specs=(act_spec, act_spec, weight_spec, weight_spec, weight_spec), out_specs=(act_spec, weight_spec, weight_spec, weight_spec), check_vma=False)
```

```python
import jax
import jax.numpy as jnp
from jax import lax
from jax.experimental import pallas as pl
from jax.experimental.pallas import tpu as pltpu
from jax.sharding import PartitionSpec as P

EPS = 1e-6
BF = jnp.bfloat16
F32 = jnp.float32
MESH = pl.DeviceIdType.MESH

NL = 4
NM = 4
OWN = 64
ROWS = 512
D = 2048
FS = 1408
F2C = 2 * FS
SPLIT = 768
ONE, TWO = 1, 2
LAST = NL - ONE
HALF = 256
QUART = 128
FAR = 4
NP = 8
NS = 7
CORES = range(TWO)
MS = 512


(S_GU, S_O, S_OWN, S_TC, S_TB, S_NEAR, S_AB, S_COL, S_ST, S_ST1, S_AB1, S_FAR, S_SX, S_H, S_H1, S_H2, S_H3, S_HL, S_SPILL, S_SPILL2) = range(20)


def mm(lhs, rhs, ld=1, rd=0):
    return lax.dot_general(lhs, rhs, (((ld,), (rd,)), ((), ())), preferred_element_type=F32)


def col_tiles(total, tile, body):
    full = total // tile

    def step(idx, carry):
        body(pl.multiple_of(idx * tile, tile), tile)
        return carry

    lax.fori_loop(0, full, step, 0)
    if total % tile:
        body(full * tile, total % tile)


def flip(v):
    return ONE - v


def home(layer):
    return layer // TWO, layer % TWO


def kernel(x_ref, g_ref, wg_ref, wu_ref, wo_ref,
           dx_ref, dwg_ref, dwu_ref, dwo_ref, WSP, WOS, WGU, WO, XALL, AB, RC, RB, WST, SX, H, DABH, SALH,
           gu, wo, nb, ab, dab, sall, part, two, tc, tb, hown, eown, nown, wst, ncol,
           ls, w_spr, w_osr, w_t2r, w_br, w_ar, w_abr, w_or, w_s, w_os, ag_b, ag_a, ag_d, ag_c0, ag_c1, ag_s, ag_s2,
           rc_r, rc_s, rb_r, rb_s, g_b, g_c, g_o, g_bs, sx_r, sx_s, dx_r, dx_s):
    d = lax.axis_index("data")
    c = lax.axis_index("stage")
    y, x = home(d)
    mate = (d, 1 - c)

    def role(layer):
        p, r = home(layer)
        al = x + r * (y - x)
        be = y + r * (x - y)
        return r, al, be

    def chip(r, al, be):
        return be * (2 - r) + al * (1 + r)

    def nbr(layer):
        r, al, be = role(layer)
        return chip(r, flip(al), be), chip(r, al, flip(be))

    def rcopy(src, dst, ssem, rsem, dev):
        return pltpu.make_async_remote_copy(src_ref=src, dst_ref=dst, send_sem=ssem, recv_sem=rsem, device_id=dev, device_id_type=MESH)

    def wait_for(region, sem):
        pltpu.make_async_copy(region, region, sem).wait()

    bar = pltpu.get_barrier_semaphore()
    for dd in range(1, 4):
        for cc in CORES:
            pl.semaphore_signal(bar, inc=1, device_id=((d + dd) % 4, cc), device_id_type=MESH)
    pl.semaphore_signal(bar, inc=1, device_id=mate, device_id_type=MESH)
    pl.semaphore_wait(bar, 7)

    def blk(ref, k, fs, lo, n):
        return ref.at[k, pl.ds(lo, n), pl.ds(pl.multiple_of(fs * FS, QUART), FS)]

    def w_dst(l, row, wi, n):
        return WGU.at[l, pl.ds(row, n), pl.ds(wi * FS, FS)]

    def w_core(l):
        p, k = home(l)
        r, al, be = role(l)
        row = pl.multiple_of(d * MS, MS)

        @pl.when(c == p)
        def _():
            for wi, ref in enumerate((wg_ref, wu_ref)):
                rcopy(blk(ref, k, chip(r, 1 - p, flip(be)), 0, MS), WSP.at[l, :, pl.ds(wi * FS, FS)], w_s.at[l, 0], w_spr.at[l], mate).start()
                rcopy(blk(ref, k, chip(r, 1 - p, be), 0, MS), w_dst(l, row, wi, MS), w_s.at[l, 0], w_t2r.at[l], mate).start()

    def w_core_o(l):
        p, k = home(l)
        r, al, be = role(l)

        @pl.when(c == p)
        def _():
            rcopy(wo_ref.at[k, pl.ds(FS // 2, FS // 2)], WOS.at[l], w_os.at[l, 2], w_osr.at[l], mate).start()

            @pl.when(al != p)
            def _():
                rcopy(wo_ref.at[k], WO.at[l], w_os.at[l, 0], w_or.at[l], (d, al)).start()

    def w_split(l, pieces=(0, 1, 2, 3)):
        p, k = home(l)
        r, al, be = role(l)
        row = pl.multiple_of(d * MS, MS)
        bn = chip(r, al, flip(be))

        def go(get):
            for half, wi in [home(q) for q in pieces]:
                rcopy(get(wi, half * HALF), w_dst(l, row + half * HALF, wi, HALF), w_s.at[l, 1], w_br.at[l, wi, half], (bn, c)).start()

        @pl.when(c == p)
        def _():
            go(lambda wi, lo: blk((wg_ref, wu_ref)[wi], k, chip(r, c, flip(be)), lo, HALF))

        @pl.when(c != p)
        def _():
            if 0 in pieces:
                wait_for(WSP.at[l], w_spr.at[l])
            go(lambda wi, lo: WSP.at[l, pl.ds(lo, HALF), pl.ds(wi * FS, FS)])

    def w_pair(l, pieces=(0, 1, 2, 3)):
        p, k = home(l)
        r, al, be = role(l)
        row = pl.multiple_of(d * MS, MS)
        an = chip(r, flip(al), be)

        def go(get):
            for half, wi in [home(q) for q in pieces]:
                rcopy(get(wi, half * HALF), w_dst(l, row + half * HALF, wi, HALF), w_s.at[l, 2], w_ar.at[l], (an, c)).start()

        @pl.when(c == p)
        def _():
            go(lambda wi, lo: blk((wg_ref, wu_ref)[wi], k, chip(r, c, be), lo, HALF))

        @pl.when(c != p)
        def _():
            if 0 in pieces:
                wait_for(WGU.at[l, pl.ds(row, MS)], w_t2r.at[l])
            go(lambda wi, lo: w_dst(l, row + lo, wi, HALF))

    def w_fwd(l, pieces=(0, 1, 2, 3)):
        r, al, be = role(l)
        an, bn = nbr(l)
        row = pl.multiple_of(bn * MS, MS)
        for half, wi in [home(q) for q in pieces]:
            src = w_dst(l, row + half * HALF, wi, HALF)
            wait_for(src, w_br.at[l, wi, half])
            rcopy(src, src, w_s.at[l, 3], w_abr.at[l], (an, c)).start()

    def w_down(l, pieces=(0, 1, 2, 3)):
        p, k = home(l)
        r, al, be = role(l)
        an = chip(r, flip(al), be)
        half, n = FS // 2, FS // 8

        @pl.when(c == p)
        def _():
            for q in pieces:
                rcopy(wo_ref.at[k, pl.ds(q * n, n)], WO.at[l, pl.ds(q * n, n)], w_os.at[l, 1], w_or.at[l], (an, al)).start()

        @pl.when(c != p)
        def _():
            if 0 in pieces:
                wait_for(WOS.at[l], w_osr.at[l])
            for q in pieces:
                rcopy(WOS.at[l, pl.ds(q * n, n)], WO.at[l, pl.ds(half + q * n, n)], w_os.at[l, 1], w_or.at[l], (an, al)).start()

    def w_wait_gu(l):
        r, al, be = role(l)
        an, bn = nbr(l)
        abn = chip(r, flip(al), flip(be))

        wait_for(WGU.at[l, pl.ds(pl.multiple_of(an * MS, MS), MS)], w_ar.at[l])
        wait_for(WGU.at[l, pl.ds(pl.multiple_of(abn * MS, MS), MS)], w_abr.at[l])

    def w_wait_o(l):
        p, k = home(l)
        r, al, be = role(l)

        @pl.when(jnp.logical_not(jnp.logical_and(c == al, c == p)))
        def _():
            wait_for(WO.at[l], w_or.at[l])

    def load_gu(l):
        p, k = home(l)
        r, al, be = role(l)
        for dd in range(1, 4):
            row = pl.multiple_of(((d + dd) % 4) * MS, MS)
            pltpu.make_async_copy(WGU.at[l, pl.ds(row, MS)], gu.at[pl.ds(row, MS)], ls.at[S_GU]).start()
        row = pl.multiple_of(d * MS, MS)

        @pl.when(c == p)
        def _():
            for wi, ref in enumerate((wg_ref, wu_ref)):
                pltpu.make_async_copy(blk(ref, k, chip(r, c, be), 0, MS), gu.at[pl.ds(row, MS), pl.ds(wi * FS, FS)], ls.at[S_GU]).start()

        @pl.when(c != p)
        def _():
            pltpu.make_async_copy(WGU.at[l, pl.ds(row, MS)], gu.at[pl.ds(row, MS)], ls.at[S_GU]).start()

    def load_o(l):
        p, k = home(l)
        r, al, be = role(l)
        mine = jnp.logical_and(c == al, c == p)

        @pl.when(mine)
        def _():
            pltpu.make_async_copy(wo_ref.at[k], wo, ls.at[S_O]).start()

        @pl.when(jnp.logical_not(mine))
        def _():
            pltpu.make_async_copy(WO.at[l], wo, ls.at[S_O]).start()

    def slot(ph, m, lo, n):
        return XALL.at[ph, m, pl.ds(lo * OWN, n * OWN)]

    def lazy(ph):
        return jnp.logical_or(ph == ONE, ph == TWO)

    def ag_start(ph, layer, m, src):
        an, bn = nbr(layer)
        pltpu.make_async_copy(src, slot(ph, m, 0, ONE), ls.at[S_OWN]).start()
        rcopy(src, slot(ph, m, ONE, ONE), ag_s.at[ph, m], ag_b.at[ph, m], (bn, c)).start()

        @pl.when(jnp.logical_not(lazy(ph)))
        def _():
            rcopy(src, slot(ph, m, FAR, ONE), ag_s.at[ph, m], ag_a.at[ph, m], (an, c)).start()

        wait_for(slot(ph, m, 0, ONE), ls.at[S_OWN])

    def other_way(ph):
        return jnp.logical_or(jnp.logical_or(ph == 0, ph == LAST), jnp.logical_or(ph == NL + ONE, ph == NP - ONE))

    def ag_mid(ph, layer, m):
        an, bn = nbr(layer)
        alt = other_way(ph)
        wait_for(slot(ph, m, ONE, ONE), ag_b.at[ph, m])
        rcopy(slot(ph, m, 0, TWO), slot(ph, m, TWO, TWO), ag_s.at[ph, m], ag_c0.at[ph, m], mate).start()

        @pl.when(jnp.logical_not(jnp.logical_or(alt, lazy(ph))))
        def _():
            rcopy(slot(ph, m, ONE, ONE), slot(ph, m, FAR + ONE, ONE), ag_s.at[ph, m], ag_d.at[ph, m], (an, c)).start()

        @pl.when(alt)
        def _():
            wait_for(slot(ph, m, FAR, ONE), ag_a.at[ph, m])
            rcopy(slot(ph, m, FAR, ONE), slot(ph, m, FAR + ONE, ONE), ag_s.at[ph, m], ag_d.at[ph, m], (bn, c)).start()

    def ag_end(ph, m):
        @pl.when(jnp.logical_not(other_way(ph)))
        def _():
            wait_for(slot(ph, m, FAR, ONE), ag_a.at[ph, m])

        wait_for(slot(ph, m, FAR + ONE, ONE), ag_d.at[ph, m])
        rcopy(slot(ph, m, FAR, TWO), slot(ph, m, FAR + TWO, TWO), ag_s.at[ph, m], ag_c1.at[ph, m], mate).start()

    def far_start(ph, m):
        an, bn = nbr(ph)
        rcopy(slot(ph, m, 0, ONE), slot(ph, m, FAR, ONE), ag_s2.at[ph, m], ag_a.at[ph, m], (an, c)).start()
        rcopy(slot(ph, m, ONE, ONE), slot(ph, m, FAR + ONE, ONE), ag_s2.at[ph, m], ag_d.at[ph, m], (an, c)).start()

    def far_end(ph, m):
        wait_for(slot(ph, m, FAR, ONE), ag_a.at[ph, m])
        wait_for(slot(ph, m, FAR + ONE, ONE), ag_d.at[ph, m])
        rcopy(slot(ph, m, FAR, TWO), slot(ph, m, FAR + TWO, TWO), ag_s2.at[ph, m], ag_c1.at[ph, m], mate).start()

    def ag_load(ph, m, half):
        wait_for(slot(ph, m, 2 + 4 * half, 2), (ag_c0, ag_c1)[half].at[ph, m])
        rows = pl.ds(half * HALF, HALF)
        pltpu.make_async_copy(XALL.at[ph, m, rows], nb.at[rows], ls.at[(S_NEAR, S_FAR)[half]]).start()

    def ag_loaded(half):
        wait_for(nb.at[pl.ds(half * HALF, HALF)], ls.at[(S_NEAR, S_FAR)[half]])

    def ag_sent(ph, m):
        @pl.when(lazy(ph))
        def _():
            wait_for(slot(ph, m, 0, LAST), ag_s.at[ph, m])

        @pl.when(jnp.logical_not(lazy(ph)))
        def _():
            wait_for(slot(ph, m, 0, NS), ag_s.at[ph, m])

    def norm(h_rows):
        h_f = h_rows.astype(F32)
        inv = lax.rsqrt(jnp.mean(h_f * h_f, axis=-1, keepdims=True) + EPS)
        return h_f * inv, inv

    def rs_core(ph, m):
        rcopy(part, RC.at[ph, m], rc_s.at[ph, m], rc_r.at[ph, m], mate).start()

    def rs_load(ph, m):
        wait_for(RC.at[ph, m], rc_r.at[ph, m])
        pltpu.make_async_copy(RC.at[ph, m], tc, ls.at[S_TC]).start()

    def rs_split(ph, layer, m):
        an, bn = nbr(layer)
        wait_for(tc, ls.at[S_TC])
        two[m] = two[m] + tc[...]
        rcopy(two.at[m, pl.ds(OWN, OWN)], RB.at[ph, m], rb_s.at[ph, m], rb_r.at[ph, m], (bn, c)).start()

    def rs_total_load(ph, m):
        wait_for(RB.at[ph, m], rb_r.at[ph, m])
        pltpu.make_async_copy(RB.at[ph, m], tb, ls.at[S_TB]).start()

    def rs_total(ph, m):
        wait_for(tb, ls.at[S_TB])
        return two[m, pl.ds(0, OWN)] + tb[...]

    def rs_ready(ph, m):
        first = jnp.logical_and(ph == 0, m == 0)
        pph = jnp.where(m == 0, ph - 1, ph)
        pm = jnp.where(m == 0, NM - 1, m - 1)

        @pl.when(jnp.logical_not(first))
        def _():
            wait_for(part, rc_s.at[pph, pm])

        @pl.when(ph > 0)
        def _():
            wait_for(two.at[m, pl.ds(OWN, OWN)], rb_s.at[ph - 1, m])

    def pre(layer, m, half, store=True):
        rows = pl.ds(half * HALF, HALF)

        def tile(i, carry):
            some = pl.ds(pl.multiple_of(half * HALF + i * QUART, QUART), QUART)
            ab[some, :] = mm(nb[some, :], gu[...])
            return carry

        lax.fori_loop(0, TWO, tile, 0)
        if store:
            pltpu.make_async_copy(ab.at[rows], AB.at[layer, m, rows], ls.at[S_AB + 4 * half]).start()

    def ab_wait(half):
        wait_for(ab.at[pl.ds(half * HALF, HALF)], ls.at[S_AB + 4 * half])

    def f1_out(layer, m):
        def act(lo, n):
            a_pre = ab[pl.ds(0, HALF), pl.ds(lo, n)]
            b_pre = ab[pl.ds(0, HALF), pl.ds(lo + FS, n)]
            sall[pl.ds(0, HALF), pl.ds(lo, n)] = (a_pre * jax.nn.sigmoid(a_pre) * b_pre).astype(BF)

        col_tiles(FS, 128, act)
        rs_ready(layer, m)

        def out(lo, n):
            res = mm(sall[pl.ds(0, HALF), :], wo[:, pl.ds(lo, n)])
            two[m, :, pl.ds(lo, n)] = res[:128]
            part[:, pl.ds(lo, n)] = res[128:]

        col_tiles(D, 1024, out)
        rs_core(layer, m)

    def f3(layer, m):
        rs_total_load(layer, m)
        tot = rs_total(layer, m)
        h_new = hown[m] + tot.astype(BF)

        @pl.when(layer > 0)
        def _():
            wait_for(hown.at[m], ls.at[S_H + m])

        hown[m] = h_new

        @pl.when(layer < NL - 2)
        def _():
            pltpu.make_async_copy(hown.at[m], H.at[layer, m], ls.at[S_H + m]).start()

        n_f, inv = norm(h_new)
        ag_sent(layer, m)
        nown[m] = n_f.astype(BF)
        ag_start(layer + 1, layer + 1, m, nown.at[m])

    def b1(layer, m, half, between=None):
        rows = pl.ds(half * HALF, HALF)
        ag_loaded(half)
        t_buf = wst.at[half, :, pl.ds(0, FS)]
        t_buf[...] = mm(nb[rows, :], wo[...], ONE, ONE)
        if half:
            @pl.when(jnp.logical_not(lazy(layer)))
            def _():
                ab_wait(half)
        else:
            ab_wait(half)
        if between is not None:
            between()
        into = pl.ds(pl.multiple_of(m * ROWS + half * HALF, HALF), 256)

        def tile(lo, n):
            t_pre = t_buf[:, pl.ds(lo, n)]
            a_pre = ab[rows, pl.ds(lo, n)]
            b_pre = ab[rows, pl.ds(lo + FS, n)]
            sg = jax.nn.sigmoid(a_pre)
            silu = a_pre * sg
            sall[into, pl.ds(lo, n)] = (silu * b_pre).astype(BF)
            dab[into, pl.ds(lo, n)] = (t_pre * b_pre * sg * (1.0 + a_pre * (1.0 - sg))).astype(BF)
            dab[into, pl.ds(lo + FS, n)] = (t_pre * silu).astype(BF)

        col_tiles(FS, 128, tile)
        r, al, be = role(layer)

        @pl.when(c == al)
        def _():
            for near in CORES:
                src = pl.ds(pl.multiple_of(m * ROWS + half * HALF + near * 128, 128), QUART)
                dst = pl.ds(pl.multiple_of(m * ROWS + half * HALF + (1 - near) * 128, 128), QUART)
                rcopy(sall.at[src, pl.ds(SPLIT, FS - SPLIT)], SX.at[layer, dst], sx_s.at[layer], sx_r.at[layer], mate).start()

        @pl.when(layer > 0)
        def _():
            pltpu.make_async_copy(dab.at[into], DABH.at[layer - ONE, into], ls.at[S_SPILL]).start()
            keep = pl.ds(0, SPLIT)
            pltpu.make_async_copy(sall.at[into, keep], SALH.at[layer - ONE, into], ls.at[S_SPILL2]).start()

        more = m < LAST
        if half:
            more = jnp.logical_and(more, jnp.logical_not(lazy(layer)))

        @pl.when(more)
        def _():
            pltpu.make_async_copy(AB.at[layer, m + ONE, rows], ab.at[rows], ls.at[S_AB + 4 * half]).start()

    def b1_out(layer, m):
        ph = NS - ONE - layer
        rs_ready(ph, m)
        near = pl.ds(pl.multiple_of(m * ROWS, ROWS), 256)

        @pl.when(jnp.logical_and(m == 0, layer < LAST))
        def _():
            wait_for(gu, ls.at[S_GU])

        def out(lo, n):
            res = mm(dab[near, :], gu[pl.ds(lo, n), :], ONE, ONE)
            two[m, :, pl.ds(lo, n)] = res[:128]
            part[:, pl.ds(lo, n)] = res[128:]

        col_tiles(D, 1024, out)
        rs_core(ph, m)

    def b3(layer, m):
        q = rs_total(NS - ONE - layer, m)
        n_f, inv = norm(hown[m])
        d_res = inv * (q - n_f * jnp.mean(q * n_f, axis=-1, keepdims=True))
        e_new = (eown[m].astype(F32) + d_res).astype(BF)

        ag_sent(NL + layer, m)
        eown[m] = e_new

        @pl.when(layer > 0)
        def _():
            ag_start(NL - ONE + layer, layer - 1, m, eown.at[m])

        @pl.when(layer == 0)
        def _():
            pltpu.make_async_copy(eown.at[m], dx_ref.at[m, c], ls.at[S_OWN]).start()
            rcopy(eown.at[m], dx_ref.at[m, c], dx_s.at[m], dx_r.at[m], mate).start()
            wait_for(eown.at[m], ls.at[S_OWN])

    def grad_cols(layer, which):
        for m in range(NM):
            pltpu.make_async_copy(XALL.at[layer, m, :, pl.ds(pl.multiple_of(which * MS, MS), MS)], ncol.at[pl.ds(m * ROWS, ROWS)], ls.at[S_COL]).start()

    def w_far(layer, i):
        cols = pl.ds(pl.multiple_of(i * HALF, HALF), HALF)
        wst[i] = mm(ncol[:, cols], dab[...], 0, 0)
        pltpu.make_async_copy(wst.at[i], WST.at[layer, cols], ls.at[S_ST + i]).start()

    def w_send(layer, piece):
        p, k = home(layer)
        r, al, be = role(layer)
        an, bn = nbr(layer)
        rows = pl.ds(pl.multiple_of((piece // 2) * 64, 64), 64)
        for wi, ref in enumerate((dwg_ref, dwu_ref)):
            @pl.when(piece % 2 == wi)
            def _():
                dst = ref.at[k, rows, pl.ds(pl.multiple_of(chip(r, c, be) * FS, QUART), FS)]
                rcopy(WST.at[layer, rows, pl.ds(wi * FS, FS)], dst, g_bs.at[layer], g_b.at[layer], (bn, p)).start()

    def w_sends(layer, lo, n):
        def step(i, carry):
            w_send(layer, i)
            return carry

        lax.fori_loop(lo, lo + n, step, 0)

    def spilled(layer):
        wait_for(dab, ls.at[S_SPILL])
        wait_for(SALH.at[0], ls.at[S_SPILL2])
        x_sent(layer)

    def x_sent(layer):
        r, al, be = role(layer)

        @pl.when(c == al)
        def _():
            wait_for(SX.at[layer], sx_s.at[layer])

    def near_load(layer):
        grad_cols(layer, d)
        pltpu.make_async_copy(DABH.at[layer - ONE], dab, ls.at[S_SPILL]).start()

    def out_load(layer, again):
        r, al, be = role(layer)
        for m in range(NM):
            pltpu.make_async_copy(XALL.at[NL + layer, m], gu.at[pl.ds(m * ROWS, ROWS), pl.ds(0, D)], ls.at[S_GU]).start()

        @pl.when(c != al)
        def _():
            wait_for(SX.at[layer], sx_r.at[layer])
            pltpu.make_async_copy(SX.at[layer], sall.at[:, pl.ds(SPLIT, FS - SPLIT)], ls.at[S_SX]).start()

        @pl.when(jnp.logical_and(again, c == al))
        def _():
            pltpu.make_async_copy(SALH.at[layer - ONE], sall.at[:, pl.ds(0, SPLIT)], ls.at[S_SX]).start()

    def out_loaded(layer, again):
        r, al, be = role(layer)
        wait_for(gu.at[:, pl.ds(0, D)], ls.at[S_GU])

        @pl.when(c != al)
        def _():
            wait_for(SX.at[layer], ls.at[S_SX])

        @pl.when(jnp.logical_and(again, c == al))
        def _():
            wait_for(SALH.at[0], ls.at[S_SX])

    def w_near(layer, i):
        p, k = home(layer)
        r, al, be = role(layer)
        cols = pl.ds(pl.multiple_of(i * HALF, HALF), HALF)
        wst[i] = mm(ncol[:, cols], dab[...], 0, 0)
        for wi, ref in enumerate((dwg_ref, dwu_ref)):
            src = wst.at[i, :, pl.ds(wi * FS, FS)]
            dst = ref.at[k, cols, pl.ds(pl.multiple_of(chip(r, c, be) * FS, QUART), FS)]

            @pl.when(c == p)
            def _():
                pltpu.make_async_copy(src, dst, ls.at[S_ST + i]).start()

            @pl.when(c != p)
            def _():
                rcopy(src, dst, ls.at[S_ST + i], g_c.at[layer], (d, p)).start()

    def near_end():
        for i in CORES:
            wait_for(wst.at[i], ls.at[S_ST + i])

    def w_out(layer):
        p, k = home(layer)
        r, al, be = role(layer)
        base = jnp.where(c == al, 0, SPLIT)

        def rows_of(slot, n):
            return wst.at[slot, pl.ds(0, n), pl.ds(0, D)]

        def one(i, slot, n):
            lo = pl.multiple_of(base + i * HALF, 128)
            res = rows_of(slot, n)
            res[...] = mm(sall[:, pl.ds(lo, n)], gu[:, pl.ds(0, D)], 0, 0)
            dst = dwo_ref.at[k, pl.ds(lo, n)]

            @pl.when(c == p)
            def _():
                pltpu.make_async_copy(res, dst, ls.at[S_ST + slot]).start()

            @pl.when(c != p)
            def _():
                rcopy(res, dst, ls.at[S_ST + slot], g_o.at[layer], (d, p)).start()

        def step(i, carry):
            @pl.when(i == TWO)
            def _():
                wait_for(rows_of(0, HALF), ls.at[S_ST])

            @pl.when(jnp.logical_or(i < TWO, c == al))
            def _():
                one(i, i % TWO, HALF)

            return carry

        lax.fori_loop(0, LAST, step, 0)

        @pl.when(c == al)
        def _():
            wait_for(rows_of(0, HALF), ls.at[S_ST])

        @pl.when(c != al)
        def _():
            one(TWO, 0, QUART)
            wait_for(rows_of(0, QUART), ls.at[S_ST])

        wait_for(rows_of(ONE, HALF), ls.at[S_ST1])

    w_core(0)
    for m in range(NM):
        pltpu.make_async_copy(x_ref.at[m, c], hown.at[m], ls.at[S_TC]).start()
        pltpu.make_async_copy(g_ref.at[m, c], eown.at[m], ls.at[S_TB]).start()
    w_split(0)
    w_pair(0)
    w_core_o(0)
    wait_for(hown, ls.at[S_TC])
    wait_for(eown, ls.at[S_TB])
    for m in range(NM):
        n_f, inv = norm(hown[m])
        nown[m] = n_f.astype(BF)
        ag_start(0, 0, m, nown.at[m])
    for l in range(1, NL):
        w_core(l)
        w_core_o(l)
    w_pair(1)
    w_fwd(0)
    for m in range(NM):
        ag_mid(0, 0, m)
    w_down(0)
    w_split(1)
    w_down(1)

    def fwd_step(t, carry):
        layer, m = t // NM, t % NM

        @pl.when(m == 0)
        def _():
            w_wait_gu(layer)
            load_gu(layer)
            wait_for(gu, ls.at[S_GU])

        @pl.when(t > 0)
        def _():
            ab_wait(0)

        ag_load(layer, m, 0)
        ag_loaded(0)
        pre(layer, m, 0)

        @pl.when(jnp.logical_and(m == 0, layer < LAST))
        def _():
            w_wait_o(layer)
            load_o(layer)
            wait_for(wo, ls.at[S_O])

        @pl.when(layer < LAST)
        def _():
            f1_out(layer, m)

        @pl.when(jnp.logical_and(t >= 2, t < 14))
        def _():
            f3((t - 2) // NM, (t - 2) % NM)

        @pl.when(jnp.logical_and(t >= 3, t < 15))
        def _():
            ag_mid((t - 3) // NM + 1, (t - 3) // NM + 1, (t - 3) % NM)

        @pl.when(jnp.logical_not(lazy(layer)))
        def _():
            ag_end(layer, m)

            @pl.when(t > 0)
            def _():
                ab_wait(ONE)

            ag_load(layer, m, ONE)
            ag_loaded(ONE)
            pre(layer, m, ONE)

        @pl.when(layer < LAST)
        def _():
            rs_load(layer, m)
            rs_split(layer, layer, m)

        def at(step, *work):
            @pl.when(t == step)
            def _():
                for fn in work:
                    fn()

        def each(fn):
            for m_ in range(NM):
                fn(NP - ONE, LAST, m_)

        plan = ("F1a P2a", "F1bc P2b", "F1d S2a P2c", "S2bcd P2d", "P3ab F2a", "F2bcd P3cd D2a",
                "D2bcd D3a", "S3abcd D3b", "F3a", "F3b", "F3cd D3c", "D3d")
        sends = {"F": w_fwd, "P": w_pair, "S": w_split, "D": w_down}
        for step, words in enumerate(plan):
            for w in words.split():
                at(step, lambda: sends[w[:ONE]](int(w[ONE:TWO]), ["abcd".index(q) for q in w[TWO:]]))

        at(7, lambda: each(lambda ph, l, m_: ag_start(ph, l, m_, eown.at[m_])))
        at(9, lambda: each(ag_mid))
        at(11, lambda: each(lambda ph, l, m_: ag_end(ph, m_)))

        @pl.when(layer == LAST)
        def _():
            far_start(TWO, m)
            far_start(ONE, m)

        return carry

    lax.fori_loop(0, NL * NM, fwd_step, 0)
    ab_wait(0)
    ab_wait(1)
    w_wait_o(LAST)

    def bwd_layer(i, carry):
        layer = LAST - i
        up = layer + ONE
        ph = NS - ONE - layer
        an, bn = nbr(layer)
        late = lazy(layer)
        near = pl.ds(0, HALF)
        far = pl.ds(HALF, HALF)
        pltpu.make_async_copy(AB.at[layer, 0, near], ab.at[near], ls.at[S_AB]).start()

        @pl.when(jnp.logical_not(late))
        def _():
            pltpu.make_async_copy(AB.at[layer, 0, far], ab.at[far], ls.at[S_AB1]).start()

        load_o(layer)

        @pl.when(layer < LAST)
        def _():
            load_gu(layer)

        wait_for(wo, ls.at[S_O])

        def bulk(lyr, at, n, *only):
            for v in only:
                @pl.when(layer == v)
                def _():
                    w_sends(lyr, at, n)

        ag_load(NL + layer, 0, 0)

        @pl.when(layer < LAST)
        def _():
            spilled(up)

        def step(m, c2):
            first = jnp.logical_and(m == 0, layer < LAST)
            ag_load(jnp.where(late, layer, NL + layer), m, ONE)

            @pl.when(m == LAST)
            def _():
                grad_cols(layer, bn)

            b1(layer, m, 0)

            @pl.when(m >= TWO)
            def _():
                rs_total_load(ph, m - TWO)

            @pl.when(first)
            def _():
                rs_total_load(ph - ONE, NM - ONE)

            b1_out(layer, m)

            @pl.when(late)
            def _():
                ag_loaded(ONE)
                pre(layer, m, ONE, False)
                ag_load(NL + layer, m, ONE)

            @pl.when(first)
            def _():
                b3(up, NM - ONE)
                ag_mid(NL + layer, layer, TWO)

                @pl.when(layer > 0)
                def _():
                    pltpu.make_async_copy(H.at[layer - ONE], hown, ls.at[S_HL]).start()

                @pl.when(layer == 0)
                def _():
                    for mm_ in range(NM):
                        pltpu.make_async_copy(x_ref.at[mm_, c], hown.at[mm_], ls.at[S_HL]).start()

                wait_for(hown, ls.at[S_HL])

            @pl.when(jnp.logical_and(m == ONE, layer < LAST))
            def _():
                ag_mid(NL + layer, layer, NM - ONE)

            @pl.when(m < NM - ONE)
            def _():
                @pl.when(layer < LAST)
                def _():
                    ag_end(NL + layer, m + ONE)

                ag_load(NL + layer, m + ONE, 0)

            @pl.when(m >= TWO)
            def _():
                b3(layer, m - TWO)

            bulk(LAST, m, ONE, TWO)
            bulk(TWO, TWO * m, TWO, ONE)
            bulk(LAST, NM + TWO * m, TWO, 0)
            bulk(TWO, NP + m, ONE, 0)
            b1(layer, m, ONE, lambda: rs_load(ph, m))
            rs_split(ph, layer, m)
            return c2

        lax.fori_loop(0, NM, step, 0)
        wait_for(ncol, ls.at[S_COL])

        def far_tile(i, c2):
            w_far(layer, i)

            @pl.when(i == 0)
            def _():
                rs_total_load(ph, TWO)

                @pl.when(layer > 0)
                def _():
                    ag_mid(LAST + layer, layer - ONE, 0)

            return c2

        lax.fori_loop(0, TWO, far_tile, 0)
        b3(layer, TWO)
        near_end()

        @pl.when(layer > 0)
        def _():
            ag_mid(LAST + layer, layer - ONE, ONE)
            ag_end(LAST + layer, 0)

        @pl.when(jnp.logical_and(layer > ONE, layer < NL))
        def _():
            for m in range(NM):
                far_end(layer - ONE, m)

        return carry

    lax.fori_loop(0, NL, bwd_layer, 0)

    w_sends(0, 0, NP + NP)
    w_sends(LAST, NM + NP, NM)
    w_sends(ONE, 0, NP + NP)
    w_sends(TWO, NM + NP, NM)
    grad_cols(0, d)
    x_sent(0)
    rs_total_load(NS - ONE, LAST)

    def rest(i, carry):
        layer = (NL - i) % NL
        again = i > 0
        out_load(layer, again)
        wait_for(ncol, ls.at[S_COL])

        @pl.when(again)
        def _():
            wait_for(dab, ls.at[S_SPILL])

        def near_tile(j, c2):
            w_near(layer, j)
            return c2

        lax.fori_loop(0, TWO, near_tile, 0)

        @pl.when(i == 0)
        def _():
            b3(0, LAST)

        @pl.when(i < LAST)
        def _():
            near_load(LAST - i)

        near_end()
        out_loaded(layer, again)
        w_out(layer)
        return carry

    lax.fori_loop(0, NL, rest, 0)

    for m in range(NM):
        wait_for(dx_ref.at[m, 1 - c], dx_r.at[m])
        wait_for(dx_ref.at[m, c], dx_s.at[m])
        ag_sent(LAST, m)
        for ph in (ONE, TWO):
            wait_for(slot(ph, m, 0, FAR), ag_s2.at[ph, m])
        wait_for(two.at[m, pl.ds(OWN, OWN)], rb_s.at[6, m])
    wait_for(part, rc_s.at[6, NM - 1])
    for l in range(NL):
        p, k = home(l)
        r, al, be = role(l)
        for i in range(1, 4):
            wait_for(WGU.at[l, pl.ds(0, MS)], w_s.at[l, i])
        wait_for(WOS.at[l], w_os.at[l, 1])

        @pl.when(c == p)
        def _():
            wait_for(WGU.at[l, pl.ds(0, 2 * MS)], w_s.at[l, 0])
            wait_for(WOS.at[l], w_os.at[l, 2])

            @pl.when(al != p)
            def _():
                wait_for(WO.at[l], w_os.at[l, 0])

        wait_for(WST.at[l], g_bs.at[l])

        @pl.when(c == p)
        def _():
            wait_for(AB.at[0, pl.ds(0, 2)], g_b.at[l])
            wait_for(AB.at[0, 0], g_c.at[l])

            @pl.when(al != p)
            def _():
                wait_for(dwo_ref.at[0, pl.ds(0, SPLIT)], g_o.at[l])

            @pl.when(al == p)
            def _():
                wait_for(dwo_ref.at[0, pl.ds(0, FS - SPLIT)], g_o.at[l])


def solution(mesh):
    def body(x_loc, g_loc, gate_loc, in_loc, out_loc):
        def hbm(shape, dt):
            return jax.ShapeDtypeStruct(shape, dt)

        any_spec = pl.BlockSpec(memory_space=pl.ANY)
        dma = pltpu.SemaphoreType.DMA
        outs = (
            hbm((NM, 2, OWN, D), BF), hbm((2, MS, 4 * FS), F32), hbm((2, MS, 4 * FS), F32), hbm((2, FS, D), F32),
            hbm((NL, MS, F2C), BF), hbm((NL, FS // 2, D), BF),
            hbm((NL, D, F2C), BF), hbm((NL, FS, D), BF), hbm((NP, NM, ROWS, D), BF), hbm((NL, NM, ROWS, F2C), F32),
            hbm((NS, NM, QUART, D), F32), hbm((NS, NM, OWN, D), F32), hbm((NL, MS, F2C), F32), hbm((NL, NM * ROWS, FS - SPLIT), BF), hbm((2, NM, OWN, D), BF),
            hbm((LAST, NM * ROWS, F2C), BF), hbm((LAST, NM * ROWS, SPLIT), BF))
        scratch = [
            pltpu.VMEM((D, F2C), BF), pltpu.VMEM((FS, D), BF), pltpu.VMEM((ROWS, D), BF), pltpu.VMEM((ROWS, F2C), F32),
            pltpu.VMEM((NM * ROWS, F2C), BF), pltpu.VMEM((NM * ROWS, FS), BF), pltpu.VMEM((QUART, D), F32),
            pltpu.VMEM((NM, QUART, D), F32), pltpu.VMEM((QUART, D), F32), pltpu.VMEM((OWN, D), F32),
            pltpu.VMEM((NM, OWN, D), BF), pltpu.VMEM((NM, OWN, D), BF), pltpu.VMEM((NM, OWN, D), BF), pltpu.VMEM((2, 256, F2C), F32), pltpu.VMEM((NM * ROWS, MS), BF),
            dma((S_SPILL2 + ONE,)), dma((NL,)), dma((NL,)), dma((NL,)), dma((NL, 2, 2)), dma((NL,)), dma((NL,)), dma((NL,)), dma((NL, 4)), dma((NL, 3)),
            dma((NP, NM)), dma((NP, NM)), dma((NP, NM)), dma((NP, NM)), dma((NP, NM)), dma((NP, NM)), dma((NP, NM)),
            dma((NS, NM)), dma((NS, NM)), dma((NS, NM)), dma((NS, NM)), dma((NL,)), dma((NL,)), dma((NL,)), dma((NL,)), dma((NL,)), dma((NL,)),
            dma((NM,)), dma((NM,))]
        res = pl.pallas_call(
            kernel, out_shape=outs, in_specs=[any_spec] * 5, out_specs=(any_spec,) * len(outs), scratch_shapes=scratch,
            compiler_params=pltpu.CompilerParams(collective_id=0, has_side_effects=True, vmem_limit_bytes=67043328),
        )(x_loc.reshape(NM, 2, OWN, D), g_loc.reshape(NM, 2, OWN, D), gate_loc[0], in_loc[0], out_loc[0])
        return res[0].reshape(x_loc.shape), res[1][None], res[2][None], res[3][None]

    act_spec = P(None, "data", None, None)
    weight_spec = P("stage", None, "data", None)
    return jax.shard_map(body, mesh=mesh, in_specs=(act_spec, act_spec, weight_spec, weight_spec, weight_spec), out_specs=(act_spec, weight_spec, weight_spec, weight_spec), check_vma=False)
```

```python
import jax
import jax.numpy as jnp
from jax import lax
from jax.experimental import pallas as pl
from jax.experimental.pallas import tpu as pltpu
from jax.sharding import PartitionSpec as P

EPS = 1e-6
BF = jnp.bfloat16
F32 = jnp.float32
MESH = pl.DeviceIdType.MESH

NL = 4
NM = 4
OWN = 64
ROWS = 512
D = 2048
FS = 1408
F2C = 2 * FS
SPLIT = 768
ONE, TWO = 1, 2
LAST = NL - ONE
HALF = 256
QUART = 128
FAR = 4
NP = 8
NS = 7
CORES = range(TWO)
MS = 512


(S_GU, S_O, S_OWN, S_TC, S_TB, S_NEAR, S_AB, S_COL, S_ST, S_ST1, S_AB1, S_FAR, S_SX, S_H, S_H1, S_H2, S_H3, S_HL, S_SPILL, S_SPILL2) = range(20)


def mm(lhs, rhs, ld=1, rd=0):
    return lax.dot_general(lhs, rhs, (((ld,), (rd,)), ((), ())), preferred_element_type=F32)


def col_tiles(total, tile, body):
    full = total // tile

    def step(idx, carry):
        body(pl.multiple_of(idx * tile, tile), tile)
        return carry

    lax.fori_loop(0, full, step, 0)
    if total % tile:
        body(full * tile, total % tile)


def flip(v):
    return ONE - v


def home(layer):
    return layer // TWO, layer % TWO


def kernel(x_ref, g_ref, wg_ref, wu_ref, wo_ref,
           dx_ref, dwg_ref, dwu_ref, dwo_ref, WSP, WOS, WGU, WO, XALL, AB, RC, RB, WST, SX, H, DABH, SALH,
           gu, wo, nb, ab, dab, sall, part, two, tc, tb, hown, eown, nown, wst, ncol,
           ls, w_spr, w_osr, w_t2r, w_br, w_ar, w_abr, w_or, w_s, w_os, ag_b, ag_a, ag_d, ag_c0, ag_c1, ag_s, ag_s2,
           rc_r, rc_s, rb_r, rb_s, g_b, g_c, g_o, g_bs, sx_r, sx_s, dx_r, dx_s):
    d = lax.axis_index("data")
    c = lax.axis_index("stage")
    y, x = home(d)
    mate = (d, 1 - c)

    def role(layer):
        p, r = home(layer)
        al = x + r * (y - x)
        be = y + r * (x - y)
        return r, al, be

    def chip(r, al, be):
        return be * (2 - r) + al * (1 + r)

    def nbr(layer):
        r, al, be = role(layer)
        return chip(r, flip(al), be), chip(r, al, flip(be))

    def rcopy(src, dst, ssem, rsem, dev):
        return pltpu.make_async_remote_copy(src_ref=src, dst_ref=dst, send_sem=ssem, recv_sem=rsem, device_id=dev, device_id_type=MESH)

    def wait_for(region, sem):
        pltpu.make_async_copy(region, region, sem).wait()

    bar = pltpu.get_barrier_semaphore()
    for dd in range(1, 4):
        for cc in CORES:
            pl.semaphore_signal(bar, inc=1, device_id=((d + dd) % 4, cc), device_id_type=MESH)
    pl.semaphore_signal(bar, inc=1, device_id=mate, device_id_type=MESH)
    pl.semaphore_wait(bar, 7)

    def blk(ref, k, fs, lo, n):
        return ref.at[k, pl.ds(lo, n), pl.ds(pl.multiple_of(fs * FS, QUART), FS)]

    def w_dst(l, row, wi, n):
        return WGU.at[l, pl.ds(row, n), pl.ds(wi * FS, FS)]

    def w_core(l):
        p, k = home(l)
        r, al, be = role(l)
        row = pl.multiple_of(d * MS, MS)

        @pl.when(c == p)
        def _():
            for wi, ref in enumerate((wg_ref, wu_ref)):
                rcopy(blk(ref, k, chip(r, 1 - p, flip(be)), 0, MS), WSP.at[l, :, pl.ds(wi * FS, FS)], w_s.at[l, 0], w_spr.at[l], mate).start()
                rcopy(blk(ref, k, chip(r, 1 - p, be), 0, MS), w_dst(l, row, wi, MS), w_s.at[l, 0], w_t2r.at[l], mate).start()

    def w_core_o(l):
        p, k = home(l)
        r, al, be = role(l)

        @pl.when(c == p)
        def _():
            rcopy(wo_ref.at[k, pl.ds(FS // 2, FS // 2)], WOS.at[l], w_os.at[l, 2], w_osr.at[l], mate).start()

            @pl.when(al != p)
            def _():
                rcopy(wo_ref.at[k], WO.at[l], w_os.at[l, 0], w_or.at[l], (d, al)).start()

    def w_split(l, pieces=(0, 1, 2, 3)):
        p, k = home(l)
        r, al, be = role(l)
        row = pl.multiple_of(d * MS, MS)
        bn = chip(r, al, flip(be))

        def go(get):
            for half, wi in [home(q) for q in pieces]:
                rcopy(get(wi, half * HALF), w_dst(l, row + half * HALF, wi, HALF), w_s.at[l, 1], w_br.at[l, wi, half], (bn, c)).start()

        @pl.when(c == p)
        def _():
            go(lambda wi, lo: blk((wg_ref, wu_ref)[wi], k, chip(r, c, flip(be)), lo, HALF))

        @pl.when(c != p)
        def _():
            if 0 in pieces:
                wait_for(WSP.at[l], w_spr.at[l])
            go(lambda wi, lo: WSP.at[l, pl.ds(lo, HALF), pl.ds(wi * FS, FS)])

    def w_pair(l, pieces=(0, 1, 2, 3)):
        p, k = home(l)
        r, al, be = role(l)
        row = pl.multiple_of(d * MS, MS)
        an = chip(r, flip(al), be)

        def go(get):
            for half, wi in [home(q) for q in pieces]:
                rcopy(get(wi, half * HALF), w_dst(l, row + half * HALF, wi, HALF), w_s.at[l, 2], w_ar.at[l], (an, c)).start()

        @pl.when(c == p)
        def _():
            go(lambda wi, lo: blk((wg_ref, wu_ref)[wi], k, chip(r, c, be), lo, HALF))

        @pl.when(c != p)
        def _():
            if 0 in pieces:
                wait_for(WGU.at[l, pl.ds(row, MS)], w_t2r.at[l])
            go(lambda wi, lo: w_dst(l, row + lo, wi, HALF))

    def w_fwd(l, pieces=(0, 1, 2, 3)):
        r, al, be = role(l)
        an, bn = nbr(l)
        row = pl.multiple_of(bn * MS, MS)
        for half, wi in [home(q) for q in pieces]:
            src = w_dst(l, row + half * HALF, wi, HALF)
            wait_for(src, w_br.at[l, wi, half])
            rcopy(src, src, w_s.at[l, 3], w_abr.at[l], (an, c)).start()

    def w_down(l, pieces=(0, 1, 2, 3)):
        p, k = home(l)
        r, al, be = role(l)
        an = chip(r, flip(al), be)
        half, n = FS // 2, FS // 8

        @pl.when(c == p)
        def _():
            for q in pieces:
                rcopy(wo_ref.at[k, pl.ds(q * n, n)], WO.at[l, pl.ds(q * n, n)], w_os.at[l, 1], w_or.at[l], (an, al)).start()

        @pl.when(c != p)
        def _():
            if 0 in pieces:
                wait_for(WOS.at[l], w_osr.at[l])
            for q in pieces:
                rcopy(WOS.at[l, pl.ds(q * n, n)], WO.at[l, pl.ds(half + q * n, n)], w_os.at[l, 1], w_or.at[l], (an, al)).start()

    def w_wait_gu(l):
        r, al, be = role(l)
        an, bn = nbr(l)
        abn = chip(r, flip(al), flip(be))

        wait_for(WGU.at[l, pl.ds(pl.multiple_of(an * MS, MS), MS)], w_ar.at[l])
        wait_for(WGU.at[l, pl.ds(pl.multiple_of(abn * MS, MS), MS)], w_abr.at[l])

    def w_wait_o(l):
        p, k = home(l)
        r, al, be = role(l)

        @pl.when(jnp.logical_not(jnp.logical_and(c == al, c == p)))
        def _():
            wait_for(WO.at[l], w_or.at[l])

    def load_gu(l):
        p, k = home(l)
        r, al, be = role(l)
        for dd in range(1, 4):
            row = pl.multiple_of(((d + dd) % 4) * MS, MS)
            pltpu.make_async_copy(WGU.at[l, pl.ds(row, MS)], gu.at[pl.ds(row, MS)], ls.at[S_GU]).start()
        row = pl.multiple_of(d * MS, MS)

        @pl.when(c == p)
        def _():
            for wi, ref in enumerate((wg_ref, wu_ref)):
                pltpu.make_async_copy(blk(ref, k, chip(r, c, be), 0, MS), gu.at[pl.ds(row, MS), pl.ds(wi * FS, FS)], ls.at[S_GU]).start()

        @pl.when(c != p)
        def _():
            pltpu.make_async_copy(WGU.at[l, pl.ds(row, MS)], gu.at[pl.ds(row, MS)], ls.at[S_GU]).start()

    def load_o(l):
        p, k = home(l)
        r, al, be = role(l)
        mine = jnp.logical_and(c == al, c == p)

        @pl.when(mine)
        def _():
            pltpu.make_async_copy(wo_ref.at[k], wo, ls.at[S_O]).start()

        @pl.when(jnp.logical_not(mine))
        def _():
            pltpu.make_async_copy(WO.at[l], wo, ls.at[S_O]).start()

    def slot(ph, m, lo, n):
        return XALL.at[ph, m, pl.ds(lo * OWN, n * OWN)]

    def lazy(ph):
        return jnp.logical_or(ph == ONE, ph == TWO)

    def ag_start(ph, layer, m, src):
        an, bn = nbr(layer)
        pltpu.make_async_copy(src, slot(ph, m, 0, ONE), ls.at[S_OWN]).start()
        rcopy(src, slot(ph, m, ONE, ONE), ag_s.at[ph, m], ag_b.at[ph, m], (bn, c)).start()

        @pl.when(jnp.logical_not(lazy(ph)))
        def _():
            rcopy(src, slot(ph, m, FAR, ONE), ag_s.at[ph, m], ag_a.at[ph, m], (an, c)).start()

        wait_for(slot(ph, m, 0, ONE), ls.at[S_OWN])

    def other_way(ph):
        return jnp.logical_or(jnp.logical_or(ph == 0, ph == LAST), ph > NL)

    def ag_mid(ph, layer, m):
        an, bn = nbr(layer)
        alt = other_way(ph)
        wait_for(slot(ph, m, ONE, ONE), ag_b.at[ph, m])
        rcopy(slot(ph, m, 0, TWO), slot(ph, m, TWO, TWO), ag_s.at[ph, m], ag_c0.at[ph, m], mate).start()

        @pl.when(jnp.logical_not(jnp.logical_or(alt, lazy(ph))))
        def _():
            rcopy(slot(ph, m, ONE, ONE), slot(ph, m, FAR + ONE, ONE), ag_s.at[ph, m], ag_d.at[ph, m], (an, c)).start()

        @pl.when(alt)
        def _():
            wait_for(slot(ph, m, FAR, ONE), ag_a.at[ph, m])
            rcopy(slot(ph, m, FAR, ONE), slot(ph, m, FAR + ONE, ONE), ag_s.at[ph, m], ag_d.at[ph, m], (bn, c)).start()

    def ag_end(ph, m):
        @pl.when(jnp.logical_not(other_way(ph)))
        def _():
            wait_for(slot(ph, m, FAR, ONE), ag_a.at[ph, m])

        wait_for(slot(ph, m, FAR + ONE, ONE), ag_d.at[ph, m])
        rcopy(slot(ph, m, FAR, TWO), slot(ph, m, FAR + TWO, TWO), ag_s.at[ph, m], ag_c1.at[ph, m], mate).start()

    def far_start(ph, m):
        an, bn = nbr(ph)
        rcopy(slot(ph, m, 0, ONE), slot(ph, m, FAR, ONE), ag_s2.at[ph, m], ag_a.at[ph, m], (an, c)).start()
        rcopy(slot(ph, m, ONE, ONE), slot(ph, m, FAR + ONE, ONE), ag_s2.at[ph, m], ag_d.at[ph, m], (an, c)).start()

    def far_end(ph, m):
        wait_for(slot(ph, m, FAR, ONE), ag_a.at[ph, m])
        wait_for(slot(ph, m, FAR + ONE, ONE), ag_d.at[ph, m])
        rcopy(slot(ph, m, FAR, TWO), slot(ph, m, FAR + TWO, TWO), ag_s2.at[ph, m], ag_c1.at[ph, m], mate).start()

    def ag_load(ph, m, half):
        wait_for(slot(ph, m, 2 + 4 * half, 2), (ag_c0, ag_c1)[half].at[ph, m])
        rows = pl.ds(half * HALF, HALF)
        pltpu.make_async_copy(XALL.at[ph, m, rows], nb.at[rows], ls.at[(S_NEAR, S_FAR)[half]]).start()

    def ag_loaded(half):
        wait_for(nb.at[pl.ds(half * HALF, HALF)], ls.at[(S_NEAR, S_FAR)[half]])

    def ag_sent(ph, m):
        @pl.when(lazy(ph))
        def _():
            wait_for(slot(ph, m, 0, LAST), ag_s.at[ph, m])

        @pl.when(jnp.logical_not(lazy(ph)))
        def _():
            wait_for(slot(ph, m, 0, NS), ag_s.at[ph, m])

    def norm(h_rows):
        h_f = h_rows.astype(F32)
        inv = lax.rsqrt(jnp.mean(h_f * h_f, axis=-1, keepdims=True) + EPS)
        return h_f * inv, inv

    def rs_core(ph, m):
        rcopy(part, RC.at[ph, m], rc_s.at[ph, m], rc_r.at[ph, m], mate).start()

    def rs_load(ph, m):
        wait_for(RC.at[ph, m], rc_r.at[ph, m])
        pltpu.make_async_copy(RC.at[ph, m], tc, ls.at[S_TC]).start()

    def rs_split(ph, layer, m):
        an, bn = nbr(layer)
        wait_for(tc, ls.at[S_TC])
        two[m] = two[m] + tc[...]
        rcopy(two.at[m, pl.ds(OWN, OWN)], RB.at[ph, m], rb_s.at[ph, m], rb_r.at[ph, m], (bn, c)).start()

    def rs_total_load(ph, m):
        wait_for(RB.at[ph, m], rb_r.at[ph, m])
        pltpu.make_async_copy(RB.at[ph, m], tb, ls.at[S_TB]).start()

    def rs_total(ph, m):
        wait_for(tb, ls.at[S_TB])
        return two[m, pl.ds(0, OWN)] + tb[...]

    def rs_ready(ph, m):
        first = jnp.logical_and(ph == 0, m == 0)
        pph = jnp.where(m == 0, ph - 1, ph)
        pm = jnp.where(m == 0, NM - 1, m - 1)

        @pl.when(jnp.logical_not(first))
        def _():
            wait_for(part, rc_s.at[pph, pm])

        @pl.when(ph > 0)
        def _():
            wait_for(two.at[m, pl.ds(OWN, OWN)], rb_s.at[ph - 1, m])

    def pre(layer, m, half, store=True):
        rows = pl.ds(half * HALF, HALF)

        def tile(i, carry):
            some = pl.ds(pl.multiple_of(half * HALF + i * QUART, QUART), QUART)
            ab[some, :] = mm(nb[some, :], gu[...])
            return carry

        lax.fori_loop(0, TWO, tile, 0)
        if store:
            pltpu.make_async_copy(ab.at[rows], AB.at[layer, m, rows], ls.at[S_AB + 4 * half]).start()

    def ab_wait(half):
        wait_for(ab.at[pl.ds(half * HALF, HALF)], ls.at[S_AB + 4 * half])

    def f1_out(layer, m):
        def act(lo, n):
            a_pre = ab[pl.ds(0, HALF), pl.ds(lo, n)]
            b_pre = ab[pl.ds(0, HALF), pl.ds(lo + FS, n)]
            sall[pl.ds(0, HALF), pl.ds(lo, n)] = (a_pre * jax.nn.sigmoid(a_pre) * b_pre).astype(BF)

        col_tiles(FS, 128, act)
        rs_ready(layer, m)

        def out(lo, n):
            res = mm(sall[pl.ds(0, HALF), :], wo[:, pl.ds(lo, n)])
            two[m, :, pl.ds(lo, n)] = res[:128]
            part[:, pl.ds(lo, n)] = res[128:]

        col_tiles(D, 1024, out)
        rs_core(layer, m)

    def f3(layer, m):
        rs_total_load(layer, m)
        tot = rs_total(layer, m)
        h_new = hown[m] + tot.astype(BF)

        @pl.when(layer > 0)
        def _():
            wait_for(hown.at[m], ls.at[S_H + m])

        hown[m] = h_new

        @pl.when(layer < NL - 2)
        def _():
            pltpu.make_async_copy(hown.at[m], H.at[layer, m], ls.at[S_H + m]).start()

        n_f, inv = norm(h_new)
        ag_sent(layer, m)
        nown[m] = n_f.astype(BF)
        ag_start(layer + 1, layer + 1, m, nown.at[m])

    def b1(layer, m, half, between=None):
        rows = pl.ds(half * HALF, HALF)
        ag_loaded(half)
        t_buf = wst.at[half, :, pl.ds(0, FS)]
        t_buf[...] = mm(nb[rows, :], wo[...], ONE, ONE)
        kept = layer < LAST if half == 0 else layer == 0

        @pl.when(kept)
        def _():
            ab_wait(half)

        if between is not None:
            between()
        into = pl.ds(pl.multiple_of(m * ROWS + half * HALF, HALF), 256)

        def tile(lo, n):
            t_pre = t_buf[:, pl.ds(lo, n)]
            a_pre = ab[rows, pl.ds(lo, n)]
            b_pre = ab[rows, pl.ds(lo + FS, n)]
            sg = jax.nn.sigmoid(a_pre)
            silu = a_pre * sg
            sall[into, pl.ds(lo, n)] = (silu * b_pre).astype(BF)
            dab[into, pl.ds(lo, n)] = (t_pre * b_pre * sg * (1.0 + a_pre * (1.0 - sg))).astype(BF)
            dab[into, pl.ds(lo + FS, n)] = (t_pre * silu).astype(BF)

        col_tiles(FS, 128, tile)
        r, al, be = role(layer)

        @pl.when(c == al)
        def _():
            for near in CORES:
                src = pl.ds(pl.multiple_of(m * ROWS + half * HALF + near * 128, 128), QUART)
                dst = pl.ds(pl.multiple_of(m * ROWS + half * HALF + (1 - near) * 128, 128), QUART)
                rcopy(sall.at[src, pl.ds(SPLIT, FS - SPLIT)], SX.at[layer, dst], sx_s.at[layer], sx_r.at[layer], mate).start()

        @pl.when(layer > 0)
        def _():
            pltpu.make_async_copy(dab.at[into], DABH.at[layer - ONE, into], ls.at[S_SPILL]).start()
            keep = pl.ds(0, SPLIT)
            pltpu.make_async_copy(sall.at[into, keep], SALH.at[layer - ONE, into], ls.at[S_SPILL2]).start()

        @pl.when(jnp.logical_and(m < LAST, kept))
        def _():
            pltpu.make_async_copy(AB.at[layer, m + ONE, rows], ab.at[rows], ls.at[S_AB + 4 * half]).start()

    def b1_out(layer, m):
        ph = NS - ONE - layer
        rs_ready(ph, m)
        near = pl.ds(pl.multiple_of(m * ROWS, ROWS), 256)

        @pl.when(jnp.logical_and(m == 0, layer < LAST))
        def _():
            wait_for(gu, ls.at[S_GU])

        def out(lo, n):
            res = mm(dab[near, :], gu[pl.ds(lo, n), :], ONE, ONE)
            two[m, :, pl.ds(lo, n)] = res[:128]
            part[:, pl.ds(lo, n)] = res[128:]

        col_tiles(D, 1024, out)
        rs_core(ph, m)

    def b3(layer, m):
        q = rs_total(NS - ONE - layer, m)
        n_f, inv = norm(hown[m])
        d_res = inv * (q - n_f * jnp.mean(q * n_f, axis=-1, keepdims=True))
        e_new = (eown[m].astype(F32) + d_res).astype(BF)

        ag_sent(NL + layer, m)
        eown[m] = e_new

        @pl.when(layer > 0)
        def _():
            ag_start(NL - ONE + layer, layer - 1, m, eown.at[m])

        @pl.when(layer == 0)
        def _():
            pltpu.make_async_copy(eown.at[m], dx_ref.at[m, c], ls.at[S_OWN]).start()
            rcopy(eown.at[m], dx_ref.at[m, c], dx_s.at[m], dx_r.at[m], mate).start()
            wait_for(eown.at[m], ls.at[S_OWN])

    def grad_cols(layer, which):
        for m in range(NM):
            pltpu.make_async_copy(XALL.at[layer, m, :, pl.ds(pl.multiple_of(which * MS, MS), MS)], ncol.at[pl.ds(m * ROWS, ROWS)], ls.at[S_COL]).start()

    def w_far(layer, i):
        cols = pl.ds(pl.multiple_of(i * HALF, HALF), HALF)
        wst[i] = mm(ncol[:, cols], dab[...], 0, 0)
        pltpu.make_async_copy(wst.at[i], WST.at[layer, cols], ls.at[S_ST + i]).start()

    def w_send(layer, piece):
        p, k = home(layer)
        r, al, be = role(layer)
        an, bn = nbr(layer)
        rows = pl.ds(pl.multiple_of((piece // 2) * 64, 64), 64)
        for wi, ref in enumerate((dwg_ref, dwu_ref)):
            @pl.when(piece % 2 == wi)
            def _():
                dst = ref.at[k, rows, pl.ds(pl.multiple_of(chip(r, c, be) * FS, QUART), FS)]
                rcopy(WST.at[layer, rows, pl.ds(wi * FS, FS)], dst, g_bs.at[layer], g_b.at[layer], (bn, p)).start()

    def w_sends(layer, lo, n):
        def step(i, carry):
            w_send(layer, i)
            return carry

        lax.fori_loop(lo, lo + n, step, 0)

    def spilled(layer):
        wait_for(dab, ls.at[S_SPILL])
        wait_for(SALH.at[0], ls.at[S_SPILL2])
        x_sent(layer)

    def x_sent(layer):
        r, al, be = role(layer)

        @pl.when(c == al)
        def _():
            wait_for(SX.at[layer], sx_s.at[layer])

    def near_load(layer):
        grad_cols(layer, d)
        pltpu.make_async_copy(DABH.at[layer - ONE], dab, ls.at[S_SPILL]).start()

    def out_load(layer, again):
        r, al, be = role(layer)
        for m in range(NM):
            pltpu.make_async_copy(XALL.at[NL + layer, m], gu.at[pl.ds(m * ROWS, ROWS), pl.ds(0, D)], ls.at[S_GU]).start()

        @pl.when(c != al)
        def _():
            wait_for(SX.at[layer], sx_r.at[layer])
            pltpu.make_async_copy(SX.at[layer], sall.at[:, pl.ds(SPLIT, FS - SPLIT)], ls.at[S_SX]).start()

        @pl.when(jnp.logical_and(again, c == al))
        def _():
            pltpu.make_async_copy(SALH.at[layer - ONE], sall.at[:, pl.ds(0, SPLIT)], ls.at[S_SX]).start()

    def out_loaded(layer, again):
        r, al, be = role(layer)
        wait_for(gu.at[:, pl.ds(0, D)], ls.at[S_GU])

        @pl.when(c != al)
        def _():
            wait_for(SX.at[layer], ls.at[S_SX])

        @pl.when(jnp.logical_and(again, c == al))
        def _():
            wait_for(SALH.at[0], ls.at[S_SX])

    def w_near(layer, i):
        p, k = home(layer)
        r, al, be = role(layer)
        cols = pl.ds(pl.multiple_of(i * HALF, HALF), HALF)
        wst[i] = mm(ncol[:, cols], dab[...], 0, 0)
        for wi, ref in enumerate((dwg_ref, dwu_ref)):
            src = wst.at[i, :, pl.ds(wi * FS, FS)]
            dst = ref.at[k, cols, pl.ds(pl.multiple_of(chip(r, c, be) * FS, QUART), FS)]

            @pl.when(c == p)
            def _():
                pltpu.make_async_copy(src, dst, ls.at[S_ST + i]).start()

            @pl.when(c != p)
            def _():
                rcopy(src, dst, ls.at[S_ST + i], g_c.at[layer], (d, p)).start()

    def near_end():
        for i in CORES:
            wait_for(wst.at[i], ls.at[S_ST + i])

    def w_out(layer):
        p, k = home(layer)
        r, al, be = role(layer)
        base = jnp.where(c == al, 0, SPLIT)

        def rows_of(slot, n):
            return wst.at[slot, pl.ds(0, n), pl.ds(0, D)]

        def one(i, slot, n):
            lo = pl.multiple_of(base + i * HALF, 128)
            res = rows_of(slot, n)
            res[...] = mm(sall[:, pl.ds(lo, n)], gu[:, pl.ds(0, D)], 0, 0)
            dst = dwo_ref.at[k, pl.ds(lo, n)]

            @pl.when(c == p)
            def _():
                pltpu.make_async_copy(res, dst, ls.at[S_ST + slot]).start()

            @pl.when(c != p)
            def _():
                rcopy(res, dst, ls.at[S_ST + slot], g_o.at[layer], (d, p)).start()

        def step(i, carry):
            @pl.when(i == TWO)
            def _():
                wait_for(rows_of(0, HALF), ls.at[S_ST])

            @pl.when(jnp.logical_or(i < TWO, c == al))
            def _():
                one(i, i % TWO, HALF)

            return carry

        lax.fori_loop(0, LAST, step, 0)

        @pl.when(c == al)
        def _():
            wait_for(rows_of(0, HALF), ls.at[S_ST])

        @pl.when(c != al)
        def _():
            one(TWO, 0, QUART)
            wait_for(rows_of(0, QUART), ls.at[S_ST])

        wait_for(rows_of(ONE, HALF), ls.at[S_ST1])

    w_core(0)
    for m in range(NM):
        pltpu.make_async_copy(x_ref.at[m, c], hown.at[m], ls.at[S_TC]).start()
        pltpu.make_async_copy(g_ref.at[m, c], eown.at[m], ls.at[S_TB]).start()
    w_split(0)
    w_pair(0)
    w_core_o(0)
    wait_for(hown, ls.at[S_TC])
    wait_for(eown, ls.at[S_TB])
    for m in range(NM):
        n_f, inv = norm(hown[m])
        nown[m] = n_f.astype(BF)
        ag_start(0, 0, m, nown.at[m])
    for l in range(1, NL):
        w_core(l)
        w_core_o(l)
    w_pair(1)
    w_fwd(0)
    for m in range(NM):
        ag_mid(0, 0, m)
    w_down(0)
    w_split(1)
    w_down(1)

    def fwd_step(t, carry):
        layer, m = t // NM, t % NM

        @pl.when(m == 0)
        def _():
            w_wait_gu(layer)
            load_gu(layer)
            wait_for(gu, ls.at[S_GU])

        @pl.when(t > 0)
        def _():
            ab_wait(0)

        ag_load(layer, m, 0)
        ag_loaded(0)
        pre(layer, m, 0)

        @pl.when(jnp.logical_and(m == 0, layer < LAST))
        def _():
            w_wait_o(layer)
            load_o(layer)
            wait_for(wo, ls.at[S_O])

        @pl.when(layer < LAST)
        def _():
            f1_out(layer, m)

        @pl.when(jnp.logical_and(t >= 2, t < 14))
        def _():
            f3((t - 2) // NM, (t - 2) % NM)

        @pl.when(jnp.logical_and(t >= 3, t < 15))
        def _():
            ag_mid((t - 3) // NM + 1, (t - 3) // NM + 1, (t - 3) % NM)

        @pl.when(jnp.logical_not(lazy(layer)))
        def _():
            ag_end(layer, m)

            @pl.when(t > 0)
            def _():
                ab_wait(ONE)

            ag_load(layer, m, ONE)
            ag_loaded(ONE)
            pre(layer, m, ONE)

        @pl.when(layer < LAST)
        def _():
            rs_load(layer, m)
            rs_split(layer, layer, m)

        def at(step, *work):
            @pl.when(t == step)
            def _():
                for fn in work:
                    fn()

        def each(fn):
            for m_ in range(NM):
                fn(NP - ONE, LAST, m_)

        plan = ("F1a P2a", "F1bc P2b", "F1d S2a P2c", "S2bcd P2d", "P3ab F2a", "F2bcd P3cd D2a",
                "D2bcd D3ab", "S3abcd D3cd", "F3a", "F3b", "F3cd")
        sends = {"F": w_fwd, "P": w_pair, "S": w_split, "D": w_down}
        for step, words in enumerate(plan):
            for w in words.split():
                at(step, lambda: sends[w[:ONE]](int(w[ONE:TWO]), ["abcd".index(q) for q in w[TWO:]]))

        at(7, lambda: each(lambda ph, l, m_: ag_start(ph, l, m_, eown.at[m_])))
        at(9, lambda: each(ag_mid))
        at(11, lambda: each(lambda ph, l, m_: ag_end(ph, m_)))

        return carry

    lax.fori_loop(0, LAST * NM, fwd_step, 0)
    ab_wait(0)
    ab_wait(ONE)
    w_wait_gu(LAST)
    load_gu(LAST)
    w_wait_o(LAST)
    wait_for(gu, ls.at[S_GU])

    def layer_loads(layer):
        near = pl.ds(0, HALF)
        far = pl.ds(HALF, HALF)
        load_o(layer)

        @pl.when(layer < LAST)
        def _():
            pltpu.make_async_copy(AB.at[layer, 0, near], ab.at[near], ls.at[S_AB]).start()
            load_gu(layer)

        @pl.when(layer == 0)
        def _():
            pltpu.make_async_copy(AB.at[layer, 0, far], ab.at[far], ls.at[S_AB1]).start()

    layer_loads(LAST)

    def bwd_layer(i, carry):
        layer = LAST - i
        up = layer + ONE
        ph = NS - ONE - layer
        an, bn = nbr(layer)
        late = layer > 0

        def bulk(lyr, at, n, *only):
            for v in only:
                @pl.when(layer == v)
                def _():
                    w_sends(lyr, at, n)

        wait_for(wo, ls.at[S_O])

        @pl.when(layer < LAST)
        def _():
            ag_load(NL + layer, 0, 0)
            spilled(up)

        def step(m, c2):
            first = jnp.logical_and(m == 0, layer < LAST)
            early = jnp.logical_or(m > 0, layer == LAST)

            @pl.when(layer == LAST)
            def _():
                ag_load(layer, m, 0)
                ag_loaded(0)
                pre(layer, m, 0, False)
                ag_load(NL + layer, m, 0)

                @pl.when(m < TWO)
                def _():
                    f3(TWO, m + TWO)

                @pl.when(m < LAST)
                def _():
                    ag_mid(LAST, LAST, m + ONE)

            @pl.when(lazy(layer))
            def _():
                ag_load(layer, m, ONE)

            @pl.when(jnp.logical_and(jnp.logical_not(late), early))
            def _():
                ag_load(NL + layer, m, ONE)

            b1(layer, m, 0)

            @pl.when(m >= TWO)
            def _():
                rs_total_load(ph, m - TWO)

            @pl.when(first)
            def _():
                rs_total_load(ph - ONE, NM - ONE)

            b1_out(layer, m)

            @pl.when(jnp.logical_not(early))
            def _():
                ag_end(NL + layer, 0)

            @pl.when(layer == LAST)
            def _():
                ag_end(layer, m)
                ag_load(layer, m, ONE)

            @pl.when(late)
            def _():
                ag_loaded(ONE)
                pre(layer, m, ONE, False)
                ag_load(NL + layer, m, ONE)

            @pl.when(jnp.logical_and(jnp.logical_not(late), jnp.logical_not(early)))
            def _():
                ag_load(NL + layer, m, ONE)

            @pl.when(m == LAST)
            def _():
                grad_cols(layer, bn)

            @pl.when(first)
            def _():
                b3(up, NM - ONE)
                ag_mid(NL + layer, layer, TWO)

                @pl.when(layer > 0)
                def _():
                    pltpu.make_async_copy(H.at[layer - ONE], hown, ls.at[S_HL]).start()

                @pl.when(layer == 0)
                def _():
                    for mm_ in range(NM):
                        pltpu.make_async_copy(x_ref.at[mm_, c], hown.at[mm_], ls.at[S_HL]).start()

                wait_for(hown, ls.at[S_HL])

            @pl.when(jnp.logical_and(m == ONE, layer < LAST))
            def _():
                ag_mid(NL + layer, layer, NM - ONE)

            @pl.when(jnp.logical_and(m < LAST, layer < LAST))
            def _():
                ag_end(NL + layer, m + ONE)
                ag_load(NL + layer, m + ONE, 0)

            @pl.when(m >= TWO)
            def _():
                b3(layer, m - TWO)

            bulk(LAST, 1 + 1 * m, 1, TWO)
            bulk(TWO, 1 + 2 * m, 2, ONE)
            bulk(LAST, 5 + 2 * m, 2, 0)
            bulk(TWO, 9 + 1 * m, 1, 0)
            b1(layer, m, ONE, lambda: rs_load(ph, m))
            rs_split(ph, layer, m)

            @pl.when(layer == LAST)
            def _():
                far_start(TWO, m)
                far_start(ONE, m)

            return c2

        lax.fori_loop(0, NM, step, 0)

        @pl.when(layer > 0)
        def _():
            layer_loads(layer - ONE)

        wait_for(ncol, ls.at[S_COL])

        def far_tile(i, c2):
            w_far(layer, i)

            @pl.when(i == 0)
            def _():
                rs_total_load(ph, TWO)

                @pl.when(layer > 0)
                def _():
                    ag_mid(LAST + layer, layer - ONE, 0)

            return c2

        lax.fori_loop(0, TWO, far_tile, 0)
        b3(layer, TWO)
        near_end()

        @pl.when(layer > 0)
        def _():
            ag_mid(LAST + layer, layer - ONE, ONE)

        bulk(3, 0, 1, 3)
        bulk(2, 0, 1, 2)
        bulk(1, 0, 1, 1)

        @pl.when(jnp.logical_and(layer > ONE, layer < NL))
        def _():
            for m in range(NM):
                far_end(layer - ONE, m)

        return carry

    lax.fori_loop(0, NL, bwd_layer, 0)

    w_sends(0, 0, NP + NP)
    w_sends(LAST, 13, 3)
    w_sends(ONE, 1, 15)
    w_sends(TWO, 13, 3)
    grad_cols(0, d)
    x_sent(0)
    rs_total_load(NS - ONE, LAST)

    def rest(i, carry):
        layer = (NL - i) % NL
        again = i > 0
        out_load(layer, again)
        wait_for(ncol, ls.at[S_COL])

        @pl.when(again)
        def _():
            wait_for(dab, ls.at[S_SPILL])

        def near_tile(j, c2):
            w_near(layer, j)
            return c2

        lax.fori_loop(0, TWO, near_tile, 0)

        @pl.when(i == 0)
        def _():
            b3(0, LAST)

        @pl.when(i < LAST)
        def _():
            near_load(LAST - i)

        near_end()
        out_loaded(layer, again)
        w_out(layer)
        return carry

    lax.fori_loop(0, NL, rest, 0)

    for m in range(NM):
        wait_for(dx_ref.at[m, 1 - c], dx_r.at[m])
        wait_for(dx_ref.at[m, c], dx_s.at[m])
        ag_sent(LAST, m)
        for ph in (ONE, TWO):
            wait_for(slot(ph, m, 0, FAR), ag_s2.at[ph, m])
        wait_for(two.at[m, pl.ds(OWN, OWN)], rb_s.at[6, m])
    wait_for(part, rc_s.at[6, NM - 1])
    for l in range(NL):
        p, k = home(l)
        r, al, be = role(l)
        for i in range(1, 4):
            wait_for(WGU.at[l, pl.ds(0, MS)], w_s.at[l, i])
        wait_for(WOS.at[l], w_os.at[l, 1])

        @pl.when(c == p)
        def _():
            wait_for(WGU.at[l, pl.ds(0, 2 * MS)], w_s.at[l, 0])
            wait_for(WOS.at[l], w_os.at[l, 2])

            @pl.when(al != p)
            def _():
                wait_for(WO.at[l], w_os.at[l, 0])

        wait_for(WST.at[l], g_bs.at[l])

        @pl.when(c == p)
        def _():
            wait_for(AB.at[0, pl.ds(0, 2)], g_b.at[l])
            wait_for(AB.at[0, 0], g_c.at[l])

            @pl.when(al != p)
            def _():
                wait_for(dwo_ref.at[0, pl.ds(0, SPLIT)], g_o.at[l])

            @pl.when(al == p)
            def _():
                wait_for(dwo_ref.at[0, pl.ds(0, FS - SPLIT)], g_o.at[l])


def solution(mesh):
    def body(x_loc, g_loc, gate_loc, in_loc, out_loc):
        def hbm(shape, dt):
            return jax.ShapeDtypeStruct(shape, dt)

        any_spec = pl.BlockSpec(memory_space=pl.ANY)
        dma = pltpu.SemaphoreType.DMA
        outs = (
            hbm((NM, 2, OWN, D), BF), hbm((2, MS, 4 * FS), F32), hbm((2, MS, 4 * FS), F32), hbm((2, FS, D), F32),
            hbm((NL, MS, F2C), BF), hbm((NL, FS // 2, D), BF),
            hbm((NL, D, F2C), BF), hbm((NL, FS, D), BF), hbm((NP, NM, ROWS, D), BF), hbm((NL, NM, ROWS, F2C), F32),
            hbm((NS, NM, QUART, D), F32), hbm((NS, NM, OWN, D), F32), hbm((NL, MS, F2C), F32), hbm((NL, NM * ROWS, FS - SPLIT), BF), hbm((2, NM, OWN, D), BF),
            hbm((LAST, NM * ROWS, F2C), BF), hbm((LAST, NM * ROWS, SPLIT), BF))
        scratch = [
            pltpu.VMEM((D, F2C), BF), pltpu.VMEM((FS, D), BF), pltpu.VMEM((ROWS, D), BF), pltpu.VMEM((ROWS, F2C), F32),
            pltpu.VMEM((NM * ROWS, F2C), BF), pltpu.VMEM((NM * ROWS, FS), BF), pltpu.VMEM((QUART, D), F32),
            pltpu.VMEM((NM, QUART, D), F32), pltpu.VMEM((QUART, D), F32), pltpu.VMEM((OWN, D), F32),
            pltpu.VMEM((NM, OWN, D), BF), pltpu.VMEM((NM, OWN, D), BF), pltpu.VMEM((NM, OWN, D), BF), pltpu.VMEM((2, 256, F2C), F32), pltpu.VMEM((NM * ROWS, MS), BF),
            dma((S_SPILL2 + ONE,)), dma((NL,)), dma((NL,)), dma((NL,)), dma((NL, 2, 2)), dma((NL,)), dma((NL,)), dma((NL,)), dma((NL, 4)), dma((NL, 3)),
            dma((NP, NM)), dma((NP, NM)), dma((NP, NM)), dma((NP, NM)), dma((NP, NM)), dma((NP, NM)), dma((NP, NM)),
            dma((NS, NM)), dma((NS, NM)), dma((NS, NM)), dma((NS, NM)), dma((NL,)), dma((NL,)), dma((NL,)), dma((NL,)), dma((NL,)), dma((NL,)),
            dma((NM,)), dma((NM,))]
        res = pl.pallas_call(
            kernel, out_shape=outs, in_specs=[any_spec] * 5, out_specs=(any_spec,) * len(outs), scratch_shapes=scratch,
            compiler_params=pltpu.CompilerParams(collective_id=0, has_side_effects=True, vmem_limit_bytes=67043328),
        )(x_loc.reshape(NM, 2, OWN, D), g_loc.reshape(NM, 2, OWN, D), gate_loc[0], in_loc[0], out_loc[0])
        return res[0].reshape(x_loc.shape), res[1][None], res[2][None], res[3][None]

    act_spec = P(None, "data", None, None)
    weight_spec = P("stage", None, "data", None)
    return jax.shard_map(body, mesh=mesh, in_specs=(act_spec, act_spec, weight_spec, weight_spec, weight_spec), out_specs=(act_spec, weight_spec, weight_spec, weight_spec), check_vma=False)
```

```python
import jax
import jax.numpy as jnp
from jax import lax
from jax.experimental import pallas as pl
from jax.experimental.pallas import tpu as pltpu
from jax.sharding import PartitionSpec as P

EPS = 1e-6
BF = jnp.bfloat16
F32 = jnp.float32
MESH = pl.DeviceIdType.MESH

NL = 4
NM = 4
OWN = 64
ROWS = 512
D = 2048
FS = 1408
F2C = 2 * FS
SPLIT = 768
ONE, TWO = 1, 2
LAST = NL - ONE
HALF = 256
QUART = 128
FAR = 4
NP = 8
NS = 7
CORES = range(TWO)
MS = 512


(S_GU, S_O, S_OWN, S_TC, S_TB, S_NEAR, S_AB, S_COL, S_ST, S_ST1, S_AB1, S_FAR, S_SX, S_H, S_H1, S_H2, S_H3, S_HL, S_SPILL, S_SPILL2) = range(20)


def mm(lhs, rhs, ld=1, rd=0):
    return lax.dot_general(lhs, rhs, (((ld,), (rd,)), ((), ())), preferred_element_type=F32)


def col_tiles(total, tile, body):
    full = total // tile

    def step(idx, carry):
        body(pl.multiple_of(idx * tile, tile), tile)
        return carry

    lax.fori_loop(0, full, step, 0)
    if total % tile:
        body(full * tile, total % tile)


OUT_T = 13


def flip(v):
    return ONE - v


def home(layer):
    return layer // TWO, layer % TWO


def kernel(x_ref, g_ref, wg_ref, wu_ref, wo_ref,
           dx_ref, dwg_ref, dwu_ref, dwo_ref, WSP, WOS, WGU, WO, XALL, AB, RC, RB, WST, WT0, WT1, SX, H, DABH, SALH,
           gu, wo, nb, ab, dab, sall, part, two, tc, tb, hown, eown, nown, wst, ncol,
           ls, w_spr, w_osr, w_t2r, w_br, w_ar, w_abr, w_or, w_s, w_os, ag_b, ag_a, ag_d, ag_c0, ag_c1, ag_s, ag_s2,
           rc_r, rc_s, rb_r, rb_s, g_b, g_c, g_o, g_bs, sx_r, sx_s, dx_r, dx_s):
    d = lax.axis_index("data")
    c = lax.axis_index("stage")
    y, x = home(d)
    mate = (d, 1 - c)

    def role(layer):
        p, r = home(layer)
        al = x + r * (y - x)
        be = y + r * (x - y)
        return r, al, be

    def chip(r, al, be):
        return be * (2 - r) + al * (1 + r)

    def nbr(layer):
        r, al, be = role(layer)
        return chip(r, flip(al), be), chip(r, al, flip(be))

    def rcopy(src, dst, ssem, rsem, dev):
        return pltpu.make_async_remote_copy(src_ref=src, dst_ref=dst, send_sem=ssem, recv_sem=rsem, device_id=dev, device_id_type=MESH)

    def wait_for(region, sem):
        pltpu.make_async_copy(region, region, sem).wait()

    bar = pltpu.get_barrier_semaphore()
    for dd in range(1, 4):
        for cc in CORES:
            pl.semaphore_signal(bar, inc=1, device_id=((d + dd) % 4, cc), device_id_type=MESH)
    pl.semaphore_signal(bar, inc=1, device_id=mate, device_id_type=MESH)
    pl.semaphore_wait(bar, 7)

    def blk(ref, k, fs, lo, n):
        return ref.at[k, pl.ds(lo, n), pl.ds(pl.multiple_of(fs * FS, QUART), FS)]

    def w_dst(l, row, wi, n):
        return WGU.at[l, pl.ds(row, n), pl.ds(wi * FS, FS)]

    def w_core(l):
        p, k = home(l)
        r, al, be = role(l)
        row = pl.multiple_of(d * MS, MS)

        @pl.when(c == p)
        def _():
            for wi, ref in enumerate((wg_ref, wu_ref)):
                rcopy(blk(ref, k, chip(r, 1 - p, flip(be)), 0, MS), WSP.at[l, :, pl.ds(wi * FS, FS)], w_s.at[l, 0], w_spr.at[l], mate).start()
                rcopy(blk(ref, k, chip(r, 1 - p, be), 0, MS), w_dst(l, row, wi, MS), w_s.at[l, 0], w_t2r.at[l], mate).start()

    def w_core_o(l):
        p, k = home(l)
        r, al, be = role(l)

        @pl.when(c == p)
        def _():
            rcopy(wo_ref.at[k, pl.ds(FS // 2, FS // 2)], WOS.at[l], w_os.at[l, 2], w_osr.at[l], mate).start()

            @pl.when(al != p)
            def _():
                rcopy(wo_ref.at[k], WO.at[l], w_os.at[l, 0], w_or.at[l], (d, al)).start()

    def w_split(l, pieces=(0, 1, 2, 3)):
        p, k = home(l)
        r, al, be = role(l)
        row = pl.multiple_of(d * MS, MS)
        bn = chip(r, al, flip(be))

        def go(get):
            for half, wi in [home(q) for q in pieces]:
                rcopy(get(wi, half * HALF), w_dst(l, row + half * HALF, wi, HALF), w_s.at[l, 1], w_br.at[l, wi, half], (bn, c)).start()

        @pl.when(c == p)
        def _():
            go(lambda wi, lo: blk((wg_ref, wu_ref)[wi], k, chip(r, c, flip(be)), lo, HALF))

        @pl.when(c != p)
        def _():
            if 0 in pieces:
                wait_for(WSP.at[l], w_spr.at[l])
            go(lambda wi, lo: WSP.at[l, pl.ds(lo, HALF), pl.ds(wi * FS, FS)])

    def w_pair(l, pieces=(0, 1, 2, 3)):
        p, k = home(l)
        r, al, be = role(l)
        row = pl.multiple_of(d * MS, MS)
        an = chip(r, flip(al), be)

        def go(get):
            for half, wi in [home(q) for q in pieces]:
                rcopy(get(wi, half * HALF), w_dst(l, row + half * HALF, wi, HALF), w_s.at[l, 2], w_ar.at[l], (an, c)).start()

        @pl.when(c == p)
        def _():
            go(lambda wi, lo: blk((wg_ref, wu_ref)[wi], k, chip(r, c, be), lo, HALF))

        @pl.when(c != p)
        def _():
            if 0 in pieces:
                wait_for(WGU.at[l, pl.ds(row, MS)], w_t2r.at[l])
            go(lambda wi, lo: w_dst(l, row + lo, wi, HALF))

    def w_fwd(l, pieces=(0, 1, 2, 3)):
        r, al, be = role(l)
        an, bn = nbr(l)
        row = pl.multiple_of(bn * MS, MS)
        for half, wi in [home(q) for q in pieces]:
            src = w_dst(l, row + half * HALF, wi, HALF)
            wait_for(src, w_br.at[l, wi, half])
            rcopy(src, src, w_s.at[l, 3], w_abr.at[l], (an, c)).start()

    def w_down(l, pieces=(0, 1, 2, 3)):
        p, k = home(l)
        r, al, be = role(l)
        an = chip(r, flip(al), be)
        half, n = FS // 2, FS // 8

        @pl.when(c == p)
        def _():
            for q in pieces:
                rcopy(wo_ref.at[k, pl.ds(q * n, n)], WO.at[l, pl.ds(q * n, n)], w_os.at[l, 1], w_or.at[l], (an, al)).start()

        @pl.when(c != p)
        def _():
            if 0 in pieces:
                wait_for(WOS.at[l], w_osr.at[l])
            for q in pieces:
                rcopy(WOS.at[l, pl.ds(q * n, n)], WO.at[l, pl.ds(half + q * n, n)], w_os.at[l, 1], w_or.at[l], (an, al)).start()

    def w_wait_gu(l):
        r, al, be = role(l)
        an, bn = nbr(l)
        abn = chip(r, flip(al), flip(be))

        wait_for(WGU.at[l, pl.ds(pl.multiple_of(an * MS, MS), MS)], w_ar.at[l])
        wait_for(WGU.at[l, pl.ds(pl.multiple_of(abn * MS, MS), MS)], w_abr.at[l])

    def w_wait_o(l):
        p, k = home(l)
        r, al, be = role(l)

        @pl.when(jnp.logical_not(jnp.logical_and(c == al, c == p)))
        def _():
            wait_for(WO.at[l], w_or.at[l])

    def load_gu(l):
        p, k = home(l)
        r, al, be = role(l)
        for dd in range(1, 4):
            row = pl.multiple_of(((d + dd) % 4) * MS, MS)
            pltpu.make_async_copy(WGU.at[l, pl.ds(row, MS)], gu.at[pl.ds(row, MS)], ls.at[S_GU]).start()
        row = pl.multiple_of(d * MS, MS)

        @pl.when(c == p)
        def _():
            for wi, ref in enumerate((wg_ref, wu_ref)):
                pltpu.make_async_copy(blk(ref, k, chip(r, c, be), 0, MS), gu.at[pl.ds(row, MS), pl.ds(wi * FS, FS)], ls.at[S_GU]).start()

        @pl.when(c != p)
        def _():
            pltpu.make_async_copy(WGU.at[l, pl.ds(row, MS)], gu.at[pl.ds(row, MS)], ls.at[S_GU]).start()

    def load_o(l):
        p, k = home(l)
        r, al, be = role(l)
        mine = jnp.logical_and(c == al, c == p)

        @pl.when(mine)
        def _():
            pltpu.make_async_copy(wo_ref.at[k], wo, ls.at[S_O]).start()

        @pl.when(jnp.logical_not(mine))
        def _():
            pltpu.make_async_copy(WO.at[l], wo, ls.at[S_O]).start()

    def slot(ph, m, lo, n):
        return XALL.at[ph, m, pl.ds(lo * OWN, n * OWN)]

    def lazy(ph):
        return jnp.logical_or(ph == ONE, ph == TWO)

    def ag_start(ph, layer, m, src):
        an, bn = nbr(layer)
        pltpu.make_async_copy(src, slot(ph, m, 0, ONE), ls.at[S_OWN]).start()
        rcopy(src, slot(ph, m, ONE, ONE), ag_s.at[ph, m], ag_b.at[ph, m], (bn, c)).start()

        @pl.when(jnp.logical_not(lazy(ph)))
        def _():
            rcopy(src, slot(ph, m, FAR, ONE), ag_s.at[ph, m], ag_a.at[ph, m], (an, c)).start()

        wait_for(slot(ph, m, 0, ONE), ls.at[S_OWN])

    def other_way(ph):
        return jnp.logical_or(jnp.logical_or(ph == 0, ph == LAST), ph > NL)

    def ag_mid(ph, layer, m):
        an, bn = nbr(layer)
        alt = other_way(ph)
        wait_for(slot(ph, m, ONE, ONE), ag_b.at[ph, m])
        rcopy(slot(ph, m, 0, TWO), slot(ph, m, TWO, TWO), ag_s.at[ph, m], ag_c0.at[ph, m], mate).start()

        @pl.when(jnp.logical_not(jnp.logical_or(alt, lazy(ph))))
        def _():
            rcopy(slot(ph, m, ONE, ONE), slot(ph, m, FAR + ONE, ONE), ag_s.at[ph, m], ag_d.at[ph, m], (an, c)).start()

        @pl.when(alt)
        def _():
            wait_for(slot(ph, m, FAR, ONE), ag_a.at[ph, m])
            rcopy(slot(ph, m, FAR, ONE), slot(ph, m, FAR + ONE, ONE), ag_s.at[ph, m], ag_d.at[ph, m], (bn, c)).start()

    def ag_end(ph, m):
        @pl.when(jnp.logical_not(other_way(ph)))
        def _():
            wait_for(slot(ph, m, FAR, ONE), ag_a.at[ph, m])

        wait_for(slot(ph, m, FAR + ONE, ONE), ag_d.at[ph, m])
        rcopy(slot(ph, m, FAR, TWO), slot(ph, m, FAR + TWO, TWO), ag_s.at[ph, m], ag_c1.at[ph, m], mate).start()

    def far_start(ph, m):
        an, bn = nbr(ph)
        rcopy(slot(ph, m, 0, ONE), slot(ph, m, FAR, ONE), ag_s2.at[ph, m], ag_a.at[ph, m], (an, c)).start()
        rcopy(slot(ph, m, ONE, ONE), slot(ph, m, FAR + ONE, ONE), ag_s2.at[ph, m], ag_d.at[ph, m], (an, c)).start()

    def far_end(ph, m):
        wait_for(slot(ph, m, FAR, ONE), ag_a.at[ph, m])
        wait_for(slot(ph, m, FAR + ONE, ONE), ag_d.at[ph, m])
        rcopy(slot(ph, m, FAR, TWO), slot(ph, m, FAR + TWO, TWO), ag_s2.at[ph, m], ag_c1.at[ph, m], mate).start()

    def ag_load(ph, m, half):
        wait_for(slot(ph, m, 2 + 4 * half, 2), (ag_c0, ag_c1)[half].at[ph, m])
        rows = pl.ds(half * HALF, HALF)
        pltpu.make_async_copy(XALL.at[ph, m, rows], nb.at[rows], ls.at[(S_NEAR, S_FAR)[half]]).start()

    def ag_loaded(half):
        wait_for(nb.at[pl.ds(half * HALF, HALF)], ls.at[(S_NEAR, S_FAR)[half]])

    def ag_sent(ph, m):
        @pl.when(lazy(ph))
        def _():
            wait_for(slot(ph, m, 0, LAST), ag_s.at[ph, m])

        @pl.when(jnp.logical_not(lazy(ph)))
        def _():
            wait_for(slot(ph, m, 0, NS), ag_s.at[ph, m])

    def norm(h_rows):
        h_f = h_rows.astype(F32)
        inv = lax.rsqrt(jnp.mean(h_f * h_f, axis=-1, keepdims=True) + EPS)
        return h_f * inv, inv

    def rs_core(ph, m):
        rcopy(part, RC.at[ph, m], rc_s.at[ph, m], rc_r.at[ph, m], mate).start()

    def rs_load(ph, m):
        wait_for(RC.at[ph, m], rc_r.at[ph, m])
        pltpu.make_async_copy(RC.at[ph, m], tc, ls.at[S_TC]).start()

    def rs_split(ph, layer, m):
        an, bn = nbr(layer)
        wait_for(tc, ls.at[S_TC])
        two[m] = two[m] + tc[...]
        rcopy(two.at[m, pl.ds(OWN, OWN)], RB.at[ph, m], rb_s.at[ph, m], rb_r.at[ph, m], (bn, c)).start()

    def rs_total_load(ph, m):
        wait_for(RB.at[ph, m], rb_r.at[ph, m])
        pltpu.make_async_copy(RB.at[ph, m], tb, ls.at[S_TB]).start()

    def rs_total(ph, m):
        wait_for(tb, ls.at[S_TB])
        return two[m, pl.ds(0, OWN)] + tb[...]

    def rs_ready(ph, m):
        first = jnp.logical_and(ph == 0, m == 0)
        pph = jnp.where(m == 0, ph - 1, ph)
        pm = jnp.where(m == 0, NM - 1, m - 1)

        @pl.when(jnp.logical_not(first))
        def _():
            wait_for(part, rc_s.at[pph, pm])

        @pl.when(ph > 0)
        def _():
            wait_for(two.at[m, pl.ds(OWN, OWN)], rb_s.at[ph - 1, m])

    def pre(layer, m, half, store=True):
        rows = pl.ds(half * HALF, HALF)

        def tile(i, carry):
            some = pl.ds(pl.multiple_of(half * HALF + i * QUART, QUART), QUART)
            ab[some, :] = mm(nb[some, :], gu[...])
            return carry

        lax.fori_loop(0, TWO, tile, 0)
        if store:
            pltpu.make_async_copy(ab.at[rows], AB.at[layer, m, rows], ls.at[S_AB + 4 * half]).start()

    def ab_wait(half):
        wait_for(ab.at[pl.ds(half * HALF, HALF)], ls.at[S_AB + 4 * half])

    def f1_out(layer, m):
        def act(lo, n):
            a_pre = ab[pl.ds(0, HALF), pl.ds(lo, n)]
            b_pre = ab[pl.ds(0, HALF), pl.ds(lo + FS, n)]
            sall[pl.ds(0, HALF), pl.ds(lo, n)] = (a_pre * jax.nn.sigmoid(a_pre) * b_pre).astype(BF)

        col_tiles(FS, 128, act)
        rs_ready(layer, m)

        def out(lo, n):
            res = mm(sall[pl.ds(0, HALF), :], wo[:, pl.ds(lo, n)])
            two[m, :, pl.ds(lo, n)] = res[:128]
            part[:, pl.ds(lo, n)] = res[128:]

        col_tiles(D, 1024, out)
        rs_core(layer, m)

    def f3(layer, m):
        rs_total_load(layer, m)
        tot = rs_total(layer, m)
        h_new = hown[m] + tot.astype(BF)

        @pl.when(layer > 0)
        def _():
            wait_for(hown.at[m], ls.at[S_H + m])

        hown[m] = h_new

        @pl.when(layer < NL - 2)
        def _():
            pltpu.make_async_copy(hown.at[m], H.at[layer, m], ls.at[S_H + m]).start()

        n_f, inv = norm(h_new)
        ag_sent(layer, m)
        nown[m] = n_f.astype(BF)
        ag_start(layer + 1, layer + 1, m, nown.at[m])

    def b1(layer, m, half, between=None):
        rows = pl.ds(half * HALF, HALF)
        ag_loaded(half)
        t_buf = wst.at[half, :, pl.ds(0, FS)]
        t_buf[...] = mm(nb[rows, :], wo[...], ONE, ONE)
        kept = layer < LAST if half == 0 else layer == 0

        @pl.when(kept)
        def _():
            ab_wait(half)

        if between is not None:
            between()
        into = pl.ds(pl.multiple_of(m * ROWS + half * HALF, HALF), 256)

        def tile(lo, n):
            t_pre = t_buf[:, pl.ds(lo, n)]
            a_pre = ab[rows, pl.ds(lo, n)]
            b_pre = ab[rows, pl.ds(lo + FS, n)]
            sg = jax.nn.sigmoid(a_pre)
            silu = a_pre * sg
            sall[into, pl.ds(lo, n)] = (silu * b_pre).astype(BF)
            dab[into, pl.ds(lo, n)] = (t_pre * b_pre * sg * (1.0 + a_pre * (1.0 - sg))).astype(BF)
            dab[into, pl.ds(lo + FS, n)] = (t_pre * silu).astype(BF)

        col_tiles(FS, 128, tile)
        r, al, be = role(layer)

        @pl.when(c == al)
        def _():
            for near in CORES:
                src = pl.ds(pl.multiple_of(m * ROWS + half * HALF + near * 128, 128), QUART)
                dst = pl.ds(pl.multiple_of(m * ROWS + half * HALF + (1 - near) * 128, 128), QUART)
                rcopy(sall.at[src, pl.ds(SPLIT, FS - SPLIT)], SX.at[layer, dst], sx_s.at[layer], sx_r.at[layer], mate).start()

        @pl.when(layer > 0)
        def _():
            pltpu.make_async_copy(dab.at[into], DABH.at[layer - ONE, into], ls.at[S_SPILL]).start()
            keep = pl.ds(0, SPLIT)
            pltpu.make_async_copy(sall.at[into, keep], SALH.at[layer - ONE, into], ls.at[S_SPILL2]).start()

        @pl.when(jnp.logical_and(m < LAST, kept))
        def _():
            pltpu.make_async_copy(AB.at[layer, m + ONE, rows], ab.at[rows], ls.at[S_AB + 4 * half]).start()

    def b1_out(layer, m):
        ph = NS - ONE - layer
        rs_ready(ph, m)
        near = pl.ds(pl.multiple_of(m * ROWS, ROWS), 256)

        @pl.when(jnp.logical_and(m == 0, layer < LAST))
        def _():
            wait_for(gu, ls.at[S_GU])

        def out(lo, n):
            res = mm(dab[near, :], gu[pl.ds(lo, n), :], ONE, ONE)
            two[m, :, pl.ds(lo, n)] = res[:128]
            part[:, pl.ds(lo, n)] = res[128:]

        col_tiles(D, 1024, out)
        rs_core(ph, m)

    def b3(layer, m):
        q = rs_total(NS - ONE - layer, m)
        n_f, inv = norm(hown[m])
        d_res = inv * (q - n_f * jnp.mean(q * n_f, axis=-1, keepdims=True))
        e_new = (eown[m].astype(F32) + d_res).astype(BF)

        ag_sent(NL + layer, m)
        eown[m] = e_new

        @pl.when(layer > 0)
        def _():
            ag_start(NL - ONE + layer, layer - 1, m, eown.at[m])

        @pl.when(layer == 0)
        def _():
            pltpu.make_async_copy(eown.at[m], dx_ref.at[m, c], ls.at[S_OWN]).start()
            rcopy(eown.at[m], dx_ref.at[m, c], dx_s.at[m], dx_r.at[m], mate).start()
            wait_for(eown.at[m], ls.at[S_OWN])

    def grad_cols(layer, which):
        for m in range(NM):
            pltpu.make_async_copy(XALL.at[layer, m, :, pl.ds(pl.multiple_of(which * MS, MS), MS)], ncol.at[pl.ds(m * ROWS, ROWS)], ls.at[S_COL]).start()

    def w_far(layer, i):
        cols = pl.ds(pl.multiple_of(i * HALF, HALF), HALF)
        wst[i] = mm(ncol[:, cols], dab[...], 0, 0)
        tail = jnp.logical_and(i == ONE, layer < TWO)

        @pl.when(jnp.logical_not(tail))
        def _():
            pltpu.make_async_copy(wst.at[i], WST.at[layer, cols], ls.at[S_ST + i]).start()

        for l, ref in enumerate((WT0, WT1)):
            @pl.when(jnp.logical_and(i == ONE, layer == l))
            def _():
                pltpu.make_async_copy(wst.at[i], ref, ls.at[S_ST + i]).start()

    def w_send(layer, piece):
        p, k = home(layer)
        r, al, be = role(layer)
        an, bn = nbr(layer)
        rows = pl.ds(pl.multiple_of((piece // 2) * 64, 64), 64)
        for wi, ref in enumerate((dwg_ref, dwu_ref)):
            @pl.when(piece % 2 == wi)
            def _():
                dst = ref.at[k, rows, pl.ds(pl.multiple_of(chip(r, c, be) * FS, QUART), FS)]
                rcopy(WST.at[layer, rows, pl.ds(wi * FS, FS)], dst, g_bs.at[layer], g_b.at[layer], (bn, p)).start()

    def w_sends(layer, lo, n):
        def step(i, carry):
            w_send(layer, i)
            return carry

        lax.fori_loop(lo, lo + n, step, 0)

    def spilled(layer):
        wait_for(dab, ls.at[S_SPILL])
        wait_for(SALH.at[0], ls.at[S_SPILL2])
        x_sent(layer)

    def x_sent(layer):
        r, al, be = role(layer)

        @pl.when(c == al)
        def _():
            wait_for(SX.at[layer], sx_s.at[layer])

    def near_load(layer):
        grad_cols(layer, d)
        pltpu.make_async_copy(DABH.at[layer - ONE], dab, ls.at[S_SPILL]).start()

    def out_load(layer, again):
        r, al, be = role(layer)
        for m in range(NM):
            pltpu.make_async_copy(XALL.at[NL + layer, m], gu.at[pl.ds(m * ROWS, ROWS), pl.ds(0, D)], ls.at[S_GU]).start()

        @pl.when(c != al)
        def _():
            wait_for(SX.at[layer], sx_r.at[layer])
            pltpu.make_async_copy(SX.at[layer], sall.at[:, pl.ds(SPLIT, FS - SPLIT)], ls.at[S_SX]).start()

        @pl.when(jnp.logical_and(again, c == al))
        def _():
            pltpu.make_async_copy(SALH.at[layer - ONE], sall.at[:, pl.ds(0, SPLIT)], ls.at[S_SX]).start()

    def out_loaded(layer, again):
        r, al, be = role(layer)
        wait_for(gu.at[:, pl.ds(0, D)], ls.at[S_GU])

        @pl.when(c != al)
        def _():
            wait_for(SX.at[layer], ls.at[S_SX])

        @pl.when(jnp.logical_and(again, c == al))
        def _():
            wait_for(SALH.at[0], ls.at[S_SX])

    def w_near(layer, i):
        p, k = home(layer)
        r, al, be = role(layer)
        cols = pl.ds(pl.multiple_of(i * HALF, HALF), HALF)
        wst[i] = mm(ncol[:, cols], dab[...], 0, 0)
        for wi, ref in enumerate((dwg_ref, dwu_ref)):
            src = wst.at[i, :, pl.ds(wi * FS, FS)]
            dst = ref.at[k, cols, pl.ds(pl.multiple_of(chip(r, c, be) * FS, QUART), FS)]

            @pl.when(c == p)
            def _():
                pltpu.make_async_copy(src, dst, ls.at[S_ST + i]).start()

            @pl.when(c != p)
            def _():
                rcopy(src, dst, ls.at[S_ST + i], g_c.at[layer], (d, p)).start()

    def near_end():
        for i in CORES:
            wait_for(wst.at[i], ls.at[S_ST + i])

    def w_out(layer):
        p, k = home(layer)
        r, al, be = role(layer)
        base = jnp.where(c == al, 0, SPLIT)

        def rows_of(slot, n):
            return wst.at[slot, pl.ds(0, n), pl.ds(0, D)]

        def one(i, slot, n):
            lo = pl.multiple_of(base + i * HALF, 128)
            res = rows_of(slot, n)
            res[...] = mm(sall[:, pl.ds(lo, n)], gu[:, pl.ds(0, D)], 0, 0)
            dst = dwo_ref.at[k, pl.ds(lo, n)]

            @pl.when(c == p)
            def _():
                pltpu.make_async_copy(res, dst, ls.at[S_ST + slot]).start()

            @pl.when(c != p)
            def _():
                rcopy(res, dst, ls.at[S_ST + slot], g_o.at[layer], (d, p)).start()

        def step(i, carry):
            @pl.when(i == TWO)
            def _():
                wait_for(rows_of(0, HALF), ls.at[S_ST])

            @pl.when(jnp.logical_or(i < TWO, c == al))
            def _():
                one(i, i % TWO, HALF)

            return carry

        lax.fori_loop(0, LAST, step, 0)

        @pl.when(c == al)
        def _():
            wait_for(rows_of(0, HALF), ls.at[S_ST])

        @pl.when(c != al)
        def _():
            one(TWO, 0, QUART)
            wait_for(rows_of(0, QUART), ls.at[S_ST])

        wait_for(rows_of(ONE, HALF), ls.at[S_ST1])

    w_core(0)
    for m in range(NM):
        pltpu.make_async_copy(x_ref.at[m, c], hown.at[m], ls.at[S_TC]).start()
        pltpu.make_async_copy(g_ref.at[m, c], eown.at[m], ls.at[S_TB]).start()
    w_split(0)
    w_pair(0)
    w_core_o(0)
    wait_for(hown, ls.at[S_TC])
    wait_for(eown, ls.at[S_TB])
    for m in range(NM):
        n_f, inv = norm(hown[m])
        nown[m] = n_f.astype(BF)
        ag_start(0, 0, m, nown.at[m])
    for l in range(1, NL):
        w_core(l)
        w_core_o(l)
    w_pair(1)
    w_fwd(0)
    for m in range(NM):
        ag_mid(0, 0, m)
    w_down(0)
    w_split(1)
    w_down(1)

    def fwd_step(t, carry):
        layer, m = t // NM, t % NM

        @pl.when(m == 0)
        def _():
            w_wait_gu(layer)
            load_gu(layer)
            wait_for(gu, ls.at[S_GU])

        @pl.when(t > 0)
        def _():
            ab_wait(0)

        ag_load(layer, m, 0)
        ag_loaded(0)
        pre(layer, m, 0)

        @pl.when(jnp.logical_and(m == 0, layer < LAST))
        def _():
            w_wait_o(layer)
            load_o(layer)
            wait_for(wo, ls.at[S_O])

        @pl.when(layer < LAST)
        def _():
            f1_out(layer, m)

        @pl.when(jnp.logical_and(t >= 2, t < 14))
        def _():
            f3((t - 2) // NM, (t - 2) % NM)

        @pl.when(jnp.logical_and(t >= 3, t < 15))
        def _():
            ag_mid((t - 3) // NM + 1, (t - 3) // NM + 1, (t - 3) % NM)

        @pl.when(jnp.logical_not(lazy(layer)))
        def _():
            ag_end(layer, m)

            @pl.when(t > 0)
            def _():
                ab_wait(ONE)

            ag_load(layer, m, ONE)
            ag_loaded(ONE)
            pre(layer, m, ONE)

        @pl.when(layer < LAST)
        def _():
            rs_load(layer, m)
            rs_split(layer, layer, m)

        def at(step, *work):
            @pl.when(t == step)
            def _():
                for fn in work:
                    fn()

        def each(fn):
            for m_ in range(NM):
                fn(NP - ONE, LAST, m_)

        plan = ("F1a P2a", "F1bc P2b", "F1d S2a P2c", "S2bcd P2d", "P3ab F2a", "F2bcd P3cd D2a",
                "D2bcd D3ab", "S3abcd D3cd", "F3a", "F3b", "F3cd")
        sends = {"F": w_fwd, "P": w_pair, "S": w_split, "D": w_down}
        for step, words in enumerate(plan):
            for w in words.split():
                at(step, lambda: sends[w[:ONE]](int(w[ONE:TWO]), ["abcd".index(q) for q in w[TWO:]]))

        at(7, lambda: each(lambda ph, l, m_: ag_start(ph, l, m_, eown.at[m_])))
        at(9, lambda: each(ag_mid))
        at(11, lambda: each(lambda ph, l, m_: ag_end(ph, m_)))

        return carry

    lax.fori_loop(0, LAST * NM, fwd_step, 0)
    ab_wait(0)
    ab_wait(ONE)
    w_wait_gu(LAST)
    load_gu(LAST)
    w_wait_o(LAST)
    wait_for(gu, ls.at[S_GU])

    def layer_loads(layer):
        near = pl.ds(0, HALF)
        far = pl.ds(HALF, HALF)
        load_o(layer)

        @pl.when(layer < LAST)
        def _():
            pltpu.make_async_copy(AB.at[layer, 0, near], ab.at[near], ls.at[S_AB]).start()
            load_gu(layer)

        @pl.when(layer == 0)
        def _():
            pltpu.make_async_copy(AB.at[layer, 0, far], ab.at[far], ls.at[S_AB1]).start()

    layer_loads(LAST)

    def bwd_layer(i, carry):
        layer = LAST - i
        up = layer + ONE
        ph = NS - ONE - layer
        an, bn = nbr(layer)
        late = layer > 0

        def bulk(lyr, at, n, *only):
            for v in only:
                @pl.when(layer == v)
                def _():
                    w_sends(lyr, at, n)

        wait_for(wo, ls.at[S_O])

        @pl.when(layer < LAST)
        def _():
            ag_load(NL + layer, 0, 0)
            spilled(up)

        def step(m, c2):
            first = jnp.logical_and(m == 0, layer < LAST)
            early = jnp.logical_or(m > 0, layer == LAST)

            @pl.when(layer == LAST)
            def _():
                ag_load(layer, m, 0)
                ag_loaded(0)
                pre(layer, m, 0, False)
                ag_load(NL + layer, m, 0)

                @pl.when(m < TWO)
                def _():
                    f3(TWO, m + TWO)

                @pl.when(m < LAST)
                def _():
                    ag_mid(LAST, LAST, m + ONE)

            @pl.when(lazy(layer))
            def _():
                ag_load(layer, m, ONE)

            @pl.when(jnp.logical_and(jnp.logical_not(late), early))
            def _():
                ag_load(NL + layer, m, ONE)

            b1(layer, m, 0)

            @pl.when(m >= TWO)
            def _():
                rs_total_load(ph, m - TWO)

            @pl.when(first)
            def _():
                rs_total_load(ph - ONE, NM - ONE)

            b1_out(layer, m)

            @pl.when(jnp.logical_not(early))
            def _():
                ag_end(NL + layer, 0)

            @pl.when(layer == LAST)
            def _():
                ag_end(layer, m)
                ag_load(layer, m, ONE)

            @pl.when(late)
            def _():
                ag_loaded(ONE)
                pre(layer, m, ONE, False)
                ag_load(NL + layer, m, ONE)

            @pl.when(jnp.logical_and(jnp.logical_not(late), jnp.logical_not(early)))
            def _():
                ag_load(NL + layer, m, ONE)

            @pl.when(m == LAST)
            def _():
                grad_cols(layer, bn)

            @pl.when(first)
            def _():
                b3(up, NM - ONE)
                ag_mid(NL + layer, layer, TWO)

                @pl.when(layer > 0)
                def _():
                    pltpu.make_async_copy(H.at[layer - ONE], hown, ls.at[S_HL]).start()

                @pl.when(layer == 0)
                def _():
                    for mm_ in range(NM):
                        pltpu.make_async_copy(x_ref.at[mm_, c], hown.at[mm_], ls.at[S_HL]).start()

                wait_for(hown, ls.at[S_HL])

            @pl.when(jnp.logical_and(m == ONE, layer < LAST))
            def _():
                ag_mid(NL + layer, layer, NM - ONE)

            @pl.when(jnp.logical_and(m < LAST, layer < LAST))
            def _():
                ag_end(NL + layer, m + ONE)
                ag_load(NL + layer, m + ONE, 0)

            @pl.when(m >= TWO)
            def _():
                b3(layer, m - TWO)

            bulk(LAST, 1 + 1 * m, 1, TWO)
            bulk(TWO, 1 + 2 * m, 2, ONE)
            bulk(LAST, 5 + 2 * m, 2, 0)
            bulk(TWO, 9 + 1 * m, 1, 0)
            b1(layer, m, ONE, lambda: rs_load(ph, m))
            rs_split(ph, layer, m)

            @pl.when(layer == LAST)
            def _():
                far_start(TWO, m)
                far_start(ONE, m)

            return c2

        lax.fori_loop(0, NM, step, 0)

        @pl.when(layer > 0)
        def _():
            layer_loads(layer - ONE)

        wait_for(ncol, ls.at[S_COL])

        def far_tile(i, c2):
            w_far(layer, i)

            @pl.when(i == 0)
            def _():
                rs_total_load(ph, TWO)

                @pl.when(layer > 0)
                def _():
                    ag_mid(LAST + layer, layer - ONE, 0)

            return c2

        lax.fori_loop(0, TWO, far_tile, 0)
        b3(layer, TWO)
        near_end()

        @pl.when(layer > 0)
        def _():
            ag_mid(LAST + layer, layer - ONE, ONE)

        bulk(3, 0, 1, 3)
        bulk(2, 0, 1, 2)
        bulk(1, 0, 1, 1)

        @pl.when(jnp.logical_and(layer > ONE, layer < NL))
        def _():
            for m in range(NM):
                far_end(layer - ONE, m)

        return carry

    lax.fori_loop(0, NL, bwd_layer, 0)

    w_sends(0, 0, NP)
    w_sends(LAST, 13, 3)
    w_sends(ONE, 1, 7)
    w_sends(TWO, 13, 3)
    grad_cols(0, d)
    x_sent(0)
    rs_total_load(NS - ONE, LAST)

    def rest(i, carry):
        layer = (NL - i) % NL
        again = i > 0
        out_load(layer, again)
        wait_for(ncol, ls.at[S_COL])

        @pl.when(again)
        def _():
            wait_for(dab, ls.at[S_SPILL])

        def near_tile(j, c2):
            w_near(layer, j)
            return c2

        lax.fori_loop(0, TWO, near_tile, 0)

        @pl.when(i == 0)
        def _():
            b3(0, LAST)

        @pl.when(i < LAST)
        def _():
            near_load(LAST - i)

        near_end()
        out_loaded(layer, again)
        w_out(layer)
        return carry

    lax.fori_loop(0, NL, rest, 0)

    for m in range(NM):
        wait_for(dx_ref.at[m, 1 - c], dx_r.at[m])
        wait_for(dx_ref.at[m, c], dx_s.at[m])
        ag_sent(LAST, m)
        for ph in (ONE, TWO):
            wait_for(slot(ph, m, 0, FAR), ag_s2.at[ph, m])
        wait_for(two.at[m, pl.ds(OWN, OWN)], rb_s.at[6, m])
    wait_for(part, rc_s.at[6, NM - 1])
    for l in range(NL):
        p, k = home(l)
        r, al, be = role(l)
        for i in range(1, 4):
            wait_for(WGU.at[l, pl.ds(0, MS)], w_s.at[l, i])
        wait_for(WOS.at[l], w_os.at[l, 1])

        @pl.when(c == p)
        def _():
            wait_for(WGU.at[l, pl.ds(0, 2 * MS)], w_s.at[l, 0])
            wait_for(WOS.at[l], w_os.at[l, 2])

            @pl.when(al != p)
            def _():
                wait_for(WO.at[l], w_os.at[l, 0])

        wait_for(WST.at[l] if l >= TWO else WST.at[l, pl.ds(0, HALF)], g_bs.at[l])

        @pl.when(c == p)
        def _():
            wait_for(AB.at[0, pl.ds(0, TWO if l >= TWO else ONE)], g_b.at[l])
            wait_for(AB.at[0, 0], g_c.at[l])

            @pl.when(al != p)
            def _():
                wait_for(dwo_ref.at[0, pl.ds(0, SPLIT)], g_o.at[l])

            @pl.when(al == p)
            def _():
                wait_for(dwo_ref.at[0, pl.ds(0, FS - SPLIT)], g_o.at[l])


def solution(mesh):
    def body(x_loc, g_loc, gate_loc, in_loc, out_loc):
        def hbm(shape, dt):
            return jax.ShapeDtypeStruct(shape, dt)

        any_spec = pl.BlockSpec(memory_space=pl.ANY)
        dma = pltpu.SemaphoreType.DMA
        outs = (
            hbm((NM, 2, OWN, D), BF), hbm((2, MS, 4 * FS), F32), hbm((2, MS, 4 * FS), F32), hbm((2, FS, D), F32),
            hbm((NL, MS, F2C), BF), hbm((NL, FS // 2, D), BF),
            hbm((NL, D, F2C), BF), hbm((NL, FS, D), BF), hbm((NP, NM, ROWS, D), BF), hbm((NL, NM, ROWS, F2C), F32),
            hbm((NS, NM, QUART, D), F32), hbm((NS, NM, OWN, D), F32), hbm((NL, MS, F2C), F32), hbm((HALF, F2C), F32), hbm((HALF, F2C), F32), hbm((NL, NM * ROWS, FS - SPLIT), BF), hbm((2, NM, OWN, D), BF),
            hbm((LAST, NM * ROWS, F2C), BF), hbm((LAST, NM * ROWS, SPLIT), BF))
        scratch = [
            pltpu.VMEM((D, F2C), BF), pltpu.VMEM((FS, D), BF), pltpu.VMEM((ROWS, D), BF), pltpu.VMEM((ROWS, F2C), F32),
            pltpu.VMEM((NM * ROWS, F2C), BF), pltpu.VMEM((NM * ROWS, FS), BF), pltpu.VMEM((QUART, D), F32),
            pltpu.VMEM((NM, QUART, D), F32), pltpu.VMEM((QUART, D), F32), pltpu.VMEM((OWN, D), F32),
            pltpu.VMEM((NM, OWN, D), BF), pltpu.VMEM((NM, OWN, D), BF), pltpu.VMEM((NM, OWN, D), BF), pltpu.VMEM((2, 256, F2C), F32), pltpu.VMEM((NM * ROWS, MS), BF),
            dma((S_SPILL2 + ONE,)), dma((NL,)), dma((NL,)), dma((NL,)), dma((NL, 2, 2)), dma((NL,)), dma((NL,)), dma((NL,)), dma((NL, 4)), dma((NL, 3)),
            dma((NP, NM)), dma((NP, NM)), dma((NP, NM)), dma((NP, NM)), dma((NP, NM)), dma((NP, NM)), dma((NP, NM)),
            dma((NS, NM)), dma((NS, NM)), dma((NS, NM)), dma((NS, NM)), dma((NL,)), dma((NL,)), dma((NL,)), dma((NL,)), dma((NL,)), dma((NL,)),
            dma((NM,)), dma((NM,))]
        res = pl.pallas_call(
            kernel, out_shape=outs, in_specs=[any_spec] * 5, out_specs=(any_spec,) * len(outs), scratch_shapes=scratch,
            compiler_params=pltpu.CompilerParams(collective_id=0, has_side_effects=True, vmem_limit_bytes=67043328),
        )(x_loc.reshape(NM, 2, OWN, D), g_loc.reshape(NM, 2, OWN, D), gate_loc[0], in_loc[0], out_loc[0])
        d_idx = lax.axis_index("data")
        tails = []
        for role_, val in ((0, res[OUT_T]), (ONE, res[OUT_T + ONE])):
            for core in CORES:
                pairs = [(TWO * q + core, TWO * ((q + TWO) % NL if role_ == 0 else q + ONE - TWO * (q % TWO))) for q in range(NL)]
                tails.append(lax.ppermute(val, ("data", "stage"), pairs))
        steps = 16
        cost = pl.CostEstimate(flops=10 ** 11, bytes_accessed=10 ** 8, transcendentals=0)
        blocks = [pl.BlockSpec((ONE, 2 * MS // steps, 4 * FS), lambda i: (i // (steps // TWO), i % (steps // TWO), 0))] * TWO
        blocks.append(pl.BlockSpec((ONE, 2 * FS // steps, D), lambda i: (i // (steps // TWO), i % (steps // TWO), 0)))

        def copy(*refs):
            for src, dst in zip(refs[:LAST], refs[LAST:]):
                dst[...] = src[...]

        grads = pl.pallas_call(
            copy, grid=(steps,), out_shape=tuple(hbm(v.shape, F32) for v in res[ONE:NL]), in_specs=blocks, out_specs=tuple(blocks),
            cost_estimate=cost, compiler_params=pltpu.CompilerParams(vmem_limit_bytes=2 ** 25))(*res[ONE:NL])

        def insert(t0, t1, t2, t3, gate_in, in_in, gate_out, in_out, buf, sems):
            d = lax.axis_index("data")

            @pl.when(lax.axis_index("stage") == 0)
            def _():
                loads, stores = [], []
                for q, ref in enumerate((t0, t1, t2, t3)):
                    k, core = home(q)
                    far = d + TWO - NL * (d // TWO) if k == 0 else d + ONE - TWO * (d % TWO)
                    col = (TWO * (far // TWO) + core) if k == 0 else (TWO * core + far % TWO)
                    cols = pl.ds(pl.multiple_of(col * FS, QUART), FS)
                    loads.append(pltpu.make_async_copy(ref, buf.at[q], sems.at[q]))
                    for wi, out in enumerate((gate_out, in_out)):
                        stores.append(pltpu.make_async_copy(buf.at[q, :, pl.ds(wi * FS, FS)], out.at[k, pl.ds(HALF, HALF), cols], sems.at[NL + TWO * q + wi]))
                for cp in loads:
                    cp.start()
                for q in range(NL):
                    loads[q].wait()
                    for wi in CORES:
                        stores[TWO * q + wi].start()
                for cp in stores:
                    cp.wait()

        gate_g, in_g = pl.pallas_call(
            insert, out_shape=tuple(hbm(v.shape, F32) for v in grads[:TWO]), in_specs=[any_spec] * (NL + TWO), out_specs=(any_spec,) * TWO,
            scratch_shapes=[pltpu.VMEM((NL, HALF, F2C), F32), dma((NL + NP,))], input_output_aliases={NL: 0, NL + ONE: ONE},
            compiler_params=pltpu.CompilerParams(vmem_limit_bytes=2 ** 25))(*tails, grads[0], grads[ONE])
        return res[0].reshape(x_loc.shape), gate_g[None], in_g[None], grads[TWO][None]

    act_spec = P(None, "data", None, None)
    weight_spec = P("stage", None, "data", None)
    return jax.shard_map(body, mesh=mesh, in_specs=(act_spec, act_spec, weight_spec, weight_spec, weight_spec), out_specs=(act_spec, weight_spec, weight_spec, weight_spec), check_vma=False)
```
